32 devices in a mesh: dp: 2 (over x), tp: 16 (over z, y, core).
Axes of the slice: x: 2, y: 2, z: 4, core: 2. Of those that a mesh axis runs over, the one named last changes fastest.
Arguments:
- x_in: bfloat16 [1024, 1024], P('dp'), parts along dimension 0
- tok_pos: int32 [1024], P('dp'), parts along dimension 0
- self_k: bfloat16 [1024, 128, 16, 64], P('dp', None, 'tp'), parts along dimension 0
- self_v: bfloat16 [1024, 128, 16, 64], P('dp', None, 'tp'), parts along dimension 0
- cross_k: bfloat16 [1024, 64, 16, 64], P('dp', None, 'tp'), parts along dimension 0
- cross_v: bfloat16 [1024, 64, 16, 64], P('dp', None, 'tp'), parts along dimension 0
- enc_mask: int32 [1024, 64], P('dp'), parts along dimension 0
- rel_bias: float32 [32, 16], P(None, 'tp')
- w_q: bfloat16 [1024, 1024], P(None, 'tp')
- w_k: bfloat16 [1024, 1024], P(None, 'tp')
- w_v: bfloat16 [1024, 1024], P(None, 'tp')
- w_o: bfloat16 [1024, 1024], P('tp')
- cross_q: bfloat16 [1024, 1024], P(None, 'tp')
- cross_o: bfloat16 [1024, 1024], P('tp')
- w_gate: bfloat16 [1024, 2816], P(None, 'tp')
- w_up: bfloat16 [1024, 2816], P(None, 'tp')
- w_down: bfloat16 [2816, 1024], P('tp')
- norm_self: bfloat16 [1024], replicated
- norm_cross: bfloat16 [1024], replicated
- norm_mlp: bfloat16 [1024], replicated
Outputs:
- output 1: bfloat16 [1024, 1024], P('dp'), parts along dimension 0
- output 2: bfloat16 [1024, 128, 16, 64], P('dp', None, 'tp'), parts along dimension 0
- output 3: bfloat16 [1024, 128, 16, 64], P('dp', None, 'tp'), parts along dimension 0
There are 2 independent parts. The reference program is written for one: setup_inputs(seed, part) draws one part's arguments, and reference() takes and returns one part's arrays. A program takes and returns all parts, laid end to end along the dimension named above; an argument that names none is the same for every part.
All inputs are finite; a program needn't handle non-finite values.
Results may differ from the reference program's by a relative error of at most 0.0189546.
Values are sent between devices in bfloat16 or wider.
A program may use at most 1 GiB of HBM per device.

```python
import math
import jax
import jax.numpy as jnp
from jax import lax

BATCH_ROWS = 512
T_MAX = 128
SRC_LEN = 64
D_MODEL = 1024
N_HEADS = 16
D_HEAD = 64
D_FF = 2816

INNER_DIM = N_HEADS * D_HEAD
BUCKET_EDGES = tuple(int(math.ceil(16.0 * 8.0 ** (bucket_step / 16.0))) for bucket_step in range(1, 16))
NEG_FILL = -1e30


def draw_ends(rng_key, low_end, high_end):
    key_list = jax.random.split(rng_key, 3)
    drawn_vals = jax.random.randint(key_list[0], (BATCH_ROWS,), low_end, high_end + 1)
    high_row = jax.random.randint(key_list[1], (), 0, BATCH_ROWS)
    low_row = (high_row + jax.random.randint(key_list[2], (), 1, BATCH_ROWS)) % BATCH_ROWS
    return drawn_vals.at[high_row].set(high_end).at[low_row].set(low_end).astype(jnp.int32)


def normal_bf16(rng_key, array_shape, std_dev):
    return (std_dev * jax.random.normal(rng_key, array_shape, jnp.float32)).astype(jnp.bfloat16)


def setup_inputs(seed: int = 0, part: int = 0) -> dict:
    part_keys = jax.random.split(jax.random.fold_in(jax.random.key(seed), part), 8)
    shared_keys = jax.random.split(jax.random.key(seed + 1), 16)
    cache_shape = (BATCH_ROWS, T_MAX, N_HEADS, D_HEAD)
    cross_shape = (BATCH_ROWS, SRC_LEN, N_HEADS, D_HEAD)
    src_lens = draw_ends(part_keys[2], SRC_LEN // 4, SRC_LEN)
    bias_draw = 0.7 * jax.random.normal(shared_keys[0], (32, N_HEADS), jnp.float32)
    q_scale = (D_MODEL * D_HEAD) ** -0.5
    in_scale = D_MODEL ** -0.5
    out_scale = INNER_DIM ** -0.5
    return {
        'x_in': normal_bf16(part_keys[0], (BATCH_ROWS, D_MODEL), 1.0),
        'tok_pos': draw_ends(part_keys[1], T_MAX // 8, T_MAX - 1),
        'self_k': normal_bf16(part_keys[3], cache_shape, 1.0),
        'self_v': normal_bf16(part_keys[4], cache_shape, 1.0),
        'cross_k': normal_bf16(part_keys[5], cross_shape, 1.0),
        'cross_v': normal_bf16(part_keys[6], cross_shape, 1.0),
        'enc_mask': (jnp.arange(SRC_LEN)[None, :] < src_lens[:, None]).astype(jnp.int32),
        'rel_bias': bias_draw.at[0].add(0.5 * math.log(T_MAX) - 1.0),
        'w_q': normal_bf16(shared_keys[1], (D_MODEL, INNER_DIM), q_scale),
        'w_k': normal_bf16(shared_keys[2], (D_MODEL, INNER_DIM), in_scale),
        'w_v': normal_bf16(shared_keys[3], (D_MODEL, INNER_DIM), in_scale),
        'w_o': normal_bf16(shared_keys[4], (INNER_DIM, D_MODEL), 0.4 * math.sqrt(T_MAX) * out_scale),
        'cross_q': normal_bf16(shared_keys[5], (D_MODEL, INNER_DIM), q_scale),
        'cross_o': normal_bf16(shared_keys[6], (INNER_DIM, D_MODEL), 0.5 * math.sqrt(SRC_LEN) * out_scale),
        'w_gate': normal_bf16(shared_keys[7], (D_MODEL, D_FF), in_scale),
        'w_up': normal_bf16(shared_keys[8], (D_MODEL, D_FF), in_scale),
        'w_down': normal_bf16(shared_keys[9], (D_FF, D_MODEL), 1.5 * D_FF ** -0.5),
        'norm_self': (1.0 + 0.25 * jax.random.normal(shared_keys[10], (D_MODEL,), jnp.float32)).astype(jnp.bfloat16),
        'norm_cross': (1.0 + 0.25 * jax.random.normal(shared_keys[11], (D_MODEL,), jnp.float32)).astype(jnp.bfloat16),
        'norm_mlp': (1.0 + 0.25 * jax.random.normal(shared_keys[12], (D_MODEL,), jnp.float32)).astype(jnp.bfloat16),
    }


def rms_norm(values, norm_scale):
    inv_rms = lax.rsqrt(jnp.mean(values * values, axis=-1, keepdims=True) + 1e-6)
    return (values * inv_rms * norm_scale.astype(jnp.float32)).astype(jnp.bfloat16)


def project(normed, weight):
    return jnp.dot(normed, weight, preferred_element_type=jnp.float32).astype(jnp.bfloat16)


def rel_bucket(distance):
    bucket_edges = jnp.array(BUCKET_EDGES, dtype=jnp.int32)
    far_bucket = 16 + jnp.sum((distance[..., None] >= bucket_edges).astype(jnp.int32), axis=-1)
    return jnp.where(distance < 16, distance, far_bucket)


def attend(queries, keys_all, values_all, extra):
    def one_row(operands):
        row_q, row_k, row_v, row_extra = operands
        scores = jnp.einsum('hk,thk->ht', row_q.astype(jnp.float32), row_k.astype(jnp.float32)) + row_extra
        probs_bf = jax.nn.softmax(scores, axis=-1).astype(jnp.bfloat16)
        mixed_out = jnp.einsum('ht,thk->hk', probs_bf.astype(jnp.float32), row_v.astype(jnp.float32))
        return mixed_out.astype(jnp.bfloat16)
    return lax.map(one_row, (queries, keys_all, values_all, extra))


def reference(x_in, tok_pos, self_k, self_v, cross_k, cross_v, enc_mask, rel_bias, w_q, w_k, w_v, w_o, cross_q, cross_o, w_gate, w_up, w_down, norm_self, norm_cross, norm_mlp):
    row_count = x_in.shape[0]
    head_shape = (row_count, N_HEADS, D_HEAD)
    residual = x_in.astype(jnp.float32)
    normed = rms_norm(residual, norm_self)
    queries = project(normed, w_q).reshape(head_shape)
    new_keys = project(normed, w_k).reshape(head_shape)
    new_values = project(normed, w_v).reshape(head_shape)
    key_index = jnp.arange(T_MAX)
    at_pos = (key_index[None, :] == tok_pos[:, None])[:, :, None, None]
    new_self_k = jnp.where(at_pos, new_keys[:, None], self_k)
    new_self_v = jnp.where(at_pos, new_values[:, None], self_v)
    distance = jnp.maximum(tok_pos[:, None] - key_index[None, :], 0)
    bias_rows = jnp.swapaxes(jnp.take(rel_bias, rel_bucket(distance), axis=0), 1, 2)
    causal = (key_index[None, :] <= tok_pos[:, None])[:, None, :]
    self_extra = jnp.where(causal, bias_rows, NEG_FILL)
    mixed_self = attend(queries, new_self_k, new_self_v, self_extra)
    residual = residual + jnp.dot(mixed_self.reshape(row_count, INNER_DIM), w_o, preferred_element_type=jnp.float32)
    normed = rms_norm(residual, norm_cross)
    cross_queries = project(normed, cross_q).reshape(head_shape)
    cross_extra = jnp.where(enc_mask[:, None, :] != 0, 0.0, NEG_FILL)
    mixed_cross = attend(cross_queries, cross_k, cross_v, cross_extra)
    residual = residual + jnp.dot(mixed_cross.reshape(row_count, INNER_DIM), cross_o, preferred_element_type=jnp.float32)
    normed = rms_norm(residual, norm_mlp)
    gate_pre = jnp.dot(normed, w_gate, preferred_element_type=jnp.float32)
    up_pre = jnp.dot(normed, w_up, preferred_element_type=jnp.float32)
    hidden = (jax.nn.gelu(gate_pre, approximate=True) * up_pre).astype(jnp.bfloat16)
    residual = residual + jnp.dot(hidden, w_down, preferred_element_type=jnp.float32)
    return (residual.astype(jnp.bfloat16), new_self_k, new_self_v)
```

```python
import math
import jax
import jax.numpy as jnp
from jax import lax
from jax.experimental import pallas as pl
from jax.experimental.pallas import tpu as pltpu
from jax.sharding import PartitionSpec as P

BUCKET_EDGES = tuple(range(1, 16)) + (16,) + tuple(int(math.ceil(16.0 * 8.0 ** (m / 16.0))) for m in range(1, 16))
NEG_FILL = -1e30
MESH = pl.DeviceIdType.MESH
F32 = jnp.float32
BF16 = jnp.bfloat16
K_ORDER = (2, 1, 3)


def rms_norm(values, norm_scale):
    inv_rms = lax.rsqrt(jnp.mean(values * values, axis=-1, keepdims=True) + 1e-6)
    return (values * inv_rms * norm_scale.astype(F32)).astype(BF16)


def project(normed, weight):
    return jnp.dot(normed, weight, preferred_element_type=F32).astype(BF16)


def gelu_tanh(u):
    return u * (0.5 * (1.0 + jnp.tanh(math.sqrt(2.0 / math.pi) * (u + 0.044715 * (u * u * u)))))


def dot_nt(a, b):
    return lax.dot_general(a, b, (((1,), (1,)), ((), ())), preferred_element_type=F32)


def dot_nn(a, b):
    return jnp.dot(a, b, preferred_element_type=F32)


def tail_kernel(x_hbm, attn_ref, mask_ref, ck_hbm, cv_hbm, wo_hbm, cq_hbm, co_hbm, wg_hbm, wu_hbm, wd_hbm, nc_ref, nm_ref,
                out_ref,
                x_buf, ck, cv, wo2, cq2, co2, wg2, wu2, wd2, att_in, pair, q_snd, q_all, o_snd, o_rcv, scores,
                y_snd, y_rcv, own, z_snd, z_rcv, h_buf, act,
                loc_sem, w_ssem, w_rsem, ys_sem, yr_sem, zs_sem, zr_sem, gys_sem, gyr_sem, gzs_sem, gzr_sem, cs_sem, cr_sem):
    me = lax.axis_index("tp")
    c = lax.rem(me, 2)
    y = lax.rem(me // 2, 2)
    z = me // 4
    core_peer = {"tp": z * 4 + y * 2 + (1 - c)}
    y_peer = {"tp": z * 4 + (1 - y) * 2 + c}
    z_peer = {k: {"tp": lax.rem(z + k, 4) * 4 + y * 2 + c} for k in (1, 2, 3)}
    my_row = c * 256 + y * 128 + z * 32
    sends = []

    def remote(src, dst, ssem, rsem, peer):
        return pltpu.make_async_remote_copy(src_ref=src, dst_ref=dst, send_sem=ssem, recv_sem=rsem, device_id=peer, device_id_type=MESH)

    def start(src, dst, ssem, rsem, peer):
        copy = remote(src, dst, ssem, rsem, peer)
        copy.start()
        sends.append(copy)
        return copy

    def chunk(base, zz):
        return pl.ds(pl.multiple_of(base + zz * 32, 32), 32)

    half = wg2.shape[0] // 2
    local = [
        pltpu.make_async_copy(x_hbm.at[pl.ds(pl.multiple_of(my_row, 32), 32)], x_buf, loc_sem.at[0]),
        pltpu.make_async_copy(wo_hbm, wo2.at[pl.ds(0, 64)], loc_sem.at[1]),
        pltpu.make_async_copy(cq_hbm, cq2.at[0], loc_sem.at[2]),
        pltpu.make_async_copy(ck_hbm, ck, loc_sem.at[3]),
        pltpu.make_async_copy(cv_hbm, cv, loc_sem.at[4]),
        pltpu.make_async_copy(co_hbm, co2.at[pl.ds(0, 64)], loc_sem.at[5]),
        pltpu.make_async_copy(wg_hbm, wg2.at[pl.ds(0, half)], loc_sem.at[6]),
        pltpu.make_async_copy(wu_hbm, wu2.at[pl.ds(0, half)], loc_sem.at[7]),
        pltpu.make_async_copy(wd_hbm, wd2.at[pl.ds(0, half)], loc_sem.at[8]),
    ]
    for copy in local:
        copy.start()

    barrier = pltpu.get_barrier_semaphore()
    for peer in (core_peer, y_peer, z_peer[1], z_peer[2], z_peer[3]):
        pl.semaphore_signal(barrier, inc=1, device_id=peer, device_id_type=MESH)
    pl.semaphore_wait(barrier, 5)

    att_copy = start(attn_ref.at[pl.ds(pl.multiple_of((1 - c) * 256, 256), 256)], att_in, w_ssem.at[0], w_rsem.at[0], core_peer)
    wo_copy = start(wo_hbm, wo2.at[pl.ds(64, 64)], w_ssem.at[1], w_rsem.at[1], core_peer)
    cq_copy = start(cq_hbm, cq2.at[1], w_ssem.at[2], w_rsem.at[2], core_peer)
    co_copy = start(co_hbm, co2.at[pl.ds(64, 64)], w_ssem.at[3], w_rsem.at[3], core_peer)
    wg_copy = start(wg_hbm, wg2.at[pl.ds(half, half)], w_ssem.at[4], w_rsem.at[4], core_peer)
    wu_copy = start(wu_hbm, wu2.at[pl.ds(half, half)], w_ssem.at[5], w_rsem.at[5], core_peer)
    wd_copy = start(wd_hbm, wd2.at[pl.ds(half, half)], w_ssem.at[6], w_rsem.at[6], core_peer)

    def reduce_scatter(p, partial_of):
        y_snd[p] = partial_of((1 - y) * 128).astype(BF16)
        y_copies = {}
        for k in K_ORDER + (0,):
            zz = lax.rem(z + k, 4)
            y_copies[k] = start(y_snd.at[p, chunk(0, zz)], y_rcv.at[p, k], ys_sem.at[p, k], yr_sem.at[p, k], y_peer)
        own[...] = partial_of(y * 128)
        z_copies = {}
        for k in K_ORDER:
            zz = lax.rem(z + k, 4)
            y_copies[k].wait_recv()
            z_snd[p, k - 1] = (own[chunk(0, zz)] + y_rcv[p, k].astype(F32)).astype(BF16)
            z_copies[k] = start(z_snd.at[p, k - 1], z_rcv.at[p, k - 1], zs_sem.at[p, k - 1], zr_sem.at[p, k - 1], z_peer[k])
        y_copies[0].wait_recv()
        total = own[chunk(0, z)] + y_rcv[p, 0].astype(F32)
        for k in (1, 3, 2):
            z_copies[k].wait_recv()
            total = total + z_rcv[p, k - 1].astype(F32)
        return total

    def gather(p, buf, base):
        mine = buf.at[chunk(base + y * 128, z)]
        start(mine, mine, gys_sem.at[p, 0], gyr_sem.at[p, 0], y_peer)
        for k in K_ORDER:
            start(mine, mine, gzs_sem.at[p, k - 1], gzr_sem.at[p, k - 1], z_peer[k])

    def gathered_z(p, buf, base, k):
        part = buf.at[chunk(base + y * 128, lax.rem(z + 4 - k, 4))]
        remote(part, part, gzs_sem.at[p, k - 1], gzr_sem.at[p, k - 1], z_peer[k]).wait_recv()
        start(part, part, gys_sem.at[p, k], gyr_sem.at[p, k], y_peer)
        return part

    def gathered_y(p, buf, base, k):
        part = buf.at[chunk(base + (1 - y) * 128, lax.rem(z + 4 - k, 4))]
        remote(part, part, gys_sem.at[p, k], gyr_sem.at[p, k], y_peer).wait_recv()
        return part

    pair[:, 0:64] = attn_ref[pl.ds(pl.multiple_of(c * 256, 256), 256), :]
    att_copy.wait_recv()
    pair[:, 64:128] = att_in[...]
    local[1].wait()
    wo_copy.wait_recv()

    def rows_of(base):
        return pl.ds(pl.multiple_of(base, 128), 128)

    total = reduce_scatter(0, lambda base: dot_nn(pair[rows_of(base)], wo2[...]))
    local[0].wait()
    resid = x_buf[...].astype(F32) + total
    h_buf[0, chunk(y * 128, z)] = rms_norm(resid, nc_ref[...])
    gather(0, h_buf.at[0], 0)
    for k in (1, 3, 2):
        gathered_z(0, h_buf.at[0], 0, k)
    for k in (0, 1, 3, 2):
        gathered_y(0, h_buf.at[0], 0, k)

    cq_copy.wait_recv()
    q_snd[...] = dot_nt(cq2[1], h_buf[0]).astype(BF16)
    q_copy = start(q_snd, q_all.at[c], w_ssem.at[7], w_rsem.at[7], core_peer)
    local[2].wait()
    q_all[c] = dot_nt(cq2[0], h_buf[0]).astype(BF16)
    local[3].wait()
    local[4].wait()

    def cross(half_id):
        outs = []
        for block in range(2):
            lanes = pl.ds(pl.multiple_of(half_id * 256 + block * 128, 128), 128)
            q_blk = q_all[half_id, :, block * 128:block * 128 + 128].astype(F32)

            def score_step(i, carry):
                rows = pl.ds(pl.multiple_of(i * 8, 8), 8)
                scores[rows, :] = jnp.sum(ck[rows, :, lanes].astype(F32) * q_blk[None], axis=1)
                return carry

            lax.fori_loop(0, 8, score_step, 0)
            s = scores[...] + jnp.where(mask_ref[:, lanes] != 0, 0.0, NEG_FILL)
            e = jnp.exp(s - jnp.max(s, axis=0, keepdims=True))
            scores[...] = (e / jnp.sum(e, axis=0, keepdims=True)).astype(BF16).astype(F32)

            def mix_step(i, acc):
                rows = pl.ds(pl.multiple_of(i * 8, 8), 8)
                p_blk = scores[rows, :]
                for j in range(8):
                    acc = acc + cv[i * 8 + j, :, lanes].astype(F32) * p_blk[j:j + 1, :]
                return acc

            outs.append(lax.fori_loop(0, 8, mix_step, jnp.zeros((64, 128), F32)).astype(BF16))
        return outs

    mine = cross(c)
    q_in = remote(q_snd, q_all.at[1 - c], w_ssem.at[7], w_rsem.at[7], core_peer)
    q_in.wait_recv()
    theirs = cross(1 - c)
    for block in range(2):
        o_snd[:, block * 128:block * 128 + 128] = theirs[block]
    o_copy = start(o_snd, o_rcv, w_ssem.at[8], w_rsem.at[8], core_peer)
    for block in range(2):
        pair[block * 128:block * 128 + 128, 0:64] = mine[block].astype(F32).T.astype(BF16)
    o_copy.wait_recv()
    pair[:, 64:128] = o_rcv[...].astype(F32).T.astype(BF16)
    local[5].wait()
    co_copy.wait_recv()
    resid = resid + reduce_scatter(1, lambda base: dot_nn(pair[rows_of(base)], co2[...]))
    h_buf[1, chunk(y * 128, z)] = rms_norm(resid, nm_ref[...])
    gather(1, h_buf.at[1], 0)
    for copy in local[6:]:
        copy.wait()
    for copy in (wg_copy, wu_copy, wd_copy):
        copy.wait_recv()
    for k in (1, 3, 2):
        gathered_z(1, h_buf.at[1], 0, k)

    def mlp(base):
        h = h_buf[1, rows_of(base)]
        act[rows_of(base)] = (gelu_tanh(dot_nt(h, wg2[...])) * dot_nt(h, wu2[...])).astype(BF16)

    mlp(y * 128)
    for k in (0, 1, 3, 2):
        gathered_y(1, h_buf.at[1], 0, k)
    mlp((1 - y) * 128)
    resid = resid + reduce_scatter(2, lambda base: dot_nn(act[rows_of(base)], wd2[...]))

    out_ref[pl.ds(pl.multiple_of(my_row, 32), 32)] = resid.astype(BF16)
    gather(2, out_ref, c * 256)
    parts = [out_ref.at[chunk(c * 256 + y * 128, z)]]

    def to_core(part, slot):
        start(part, part, cs_sem.at[slot], cr_sem.at[slot], core_peer)

    to_core(parts[0], 0)
    for k in (1, 3, 2):
        to_core(gathered_z(2, out_ref, c * 256, k), k)
    for k in (0, 1, 3, 2):
        to_core(gathered_y(2, out_ref, c * 256, k), 4 + k)
    for yy in range(2):
        for k in range(4):
            base = (1 - c) * 256 + (y if yy == 0 else 1 - y) * 128
            part = out_ref.at[chunk(base, lax.rem(z + 4 - k, 4))]
            remote(part, part, cs_sem.at[yy * 4 + k], cr_sem.at[yy * 4 + k], core_peer).wait_recv()
    for copy in sends:
        copy.wait_send()


def tail(x_in, attn, mask_t, ck_t, cv_t, wo, cq_t, co, wg_t, wu_t, wd, nc, nm):
    any_spec = pl.BlockSpec(memory_space=pl.ANY)
    vmem = pl.BlockSpec(memory_space=pltpu.VMEM)
    units = wd.shape[0]
    dma = pltpu.SemaphoreType.DMA
    scratch = [
        pltpu.VMEM((32, 1024), BF16), pltpu.VMEM(ck_t.shape, BF16), pltpu.VMEM(cv_t.shape, BF16),
        pltpu.VMEM((128, 1024), BF16), pltpu.VMEM((2, 64, 1024), BF16), pltpu.VMEM((128, 1024), BF16),
        pltpu.VMEM((2 * units, 1024), BF16), pltpu.VMEM((2 * units, 1024), BF16), pltpu.VMEM((2 * units, 1024), BF16),
        pltpu.VMEM((256, 64), BF16), pltpu.VMEM((256, 128), BF16), pltpu.VMEM((64, 256), BF16), pltpu.VMEM((2, 64, 256), BF16),
        pltpu.VMEM((64, 256), BF16), pltpu.VMEM((64, 256), BF16), pltpu.VMEM((64, 128), F32),
        pltpu.VMEM((3, 128, 1024), BF16), pltpu.VMEM((3, 4, 32, 1024), BF16), pltpu.VMEM((128, 1024), F32),
        pltpu.VMEM((3, 3, 32, 1024), BF16), pltpu.VMEM((3, 3, 32, 1024), BF16), pltpu.VMEM((2, 256, 1024), BF16),
        pltpu.VMEM((256, 2 * units), BF16),
        dma((9,)), dma((9,)), dma((9,)), dma((3, 4)), dma((3, 4)), dma((3, 3)), dma((3, 3)),
        dma((3, 4)), dma((3, 4)), dma((3, 3)), dma((3, 3)), dma((8,)), dma((8,)),
    ]
    return pl.pallas_call(
        tail_kernel,
        out_shape=jax.ShapeDtypeStruct(x_in.shape, BF16),
        in_specs=[any_spec, vmem, vmem] + [any_spec] * 8 + [vmem, vmem],
        out_specs=vmem,
        scratch_shapes=scratch,
        compiler_params=pltpu.CompilerParams(collective_id=0, has_side_effects=True, vmem_limit_bytes=40 * 1024 * 1024),
        name="tail",
    )(x_in, attn, mask_t, ck_t, cv_t, wo, cq_t, co, wg_t, wu_t, wd, nc, nm)


def bias_table(rel_bias, t_len):
    distance = jnp.arange(t_len)[:, None] - jnp.arange(t_len)[None, :]
    table = jnp.full((t_len, t_len), rel_bias[0, 0], F32)
    for bucket, edge in enumerate(BUCKET_EDGES):
        table = jnp.where(distance >= edge, rel_bias[bucket + 1, 0], table)
    return table


def solution(mesh):
    def local_layer(x_in, tok_pos, self_k, self_v, cross_k, cross_v, enc_mask, rel_bias, w_q, w_k, w_v, w_o, cross_q, cross_o, w_gate, w_up, w_down, norm_self, norm_cross, norm_mlp):
        row_count, t_len, _, head_dim = self_k.shape
        normed = rms_norm(x_in.astype(F32), norm_self)
        queries = project(normed, w_q)[:, None, :]
        new_keys = project(normed, w_k)[:, None, None, :]
        new_values = project(normed, w_v)[:, None, None, :]
        key_index = jnp.arange(t_len)
        at_pos = key_index[None, :] == tok_pos[:, None]
        bias = jnp.dot(at_pos.astype(F32), bias_table(rel_bias, t_len), precision=lax.Precision.HIGHEST)
        extra = jnp.where(key_index[None, :] <= tok_pos[:, None], bias, NEG_FILL)[:, None, :]
        new_self_k = jnp.where(at_pos[:, :, None, None], new_keys, self_k)
        new_self_v = jnp.where(at_pos[:, :, None, None], new_values, self_v)
        scores = jnp.einsum('bhk,bthk->bht', queries, new_self_k, preferred_element_type=F32) + extra
        probs = jax.nn.softmax(scores, axis=-1).astype(BF16)
        mixed = jnp.einsum('bht,bthk->bhk', probs, new_self_v, preferred_element_type=F32).astype(BF16)
        attn = mixed.reshape(row_count, head_dim)
        ck_t = jnp.transpose(cross_k[:, :, 0, :], (1, 2, 0))
        cv_t = jnp.transpose(cross_v[:, :, 0, :], (1, 2, 0))
        out = tail(x_in, attn, enc_mask.T, ck_t, cv_t, w_o, cross_q.T, cross_o, w_gate.T, w_up.T, w_down,
                   norm_cross[None, :], norm_mlp[None, :])
        return out, new_self_k, new_self_v

    cache_spec = P('dp', None, 'tp', None)
    split_cols = P(None, 'tp')
    split_rows = P('tp', None)
    in_specs = (P('dp', None), P('dp'), cache_spec, cache_spec, cache_spec, cache_spec, P('dp', None), split_cols, split_cols, split_cols, split_cols, split_rows, split_cols, split_rows, split_cols, split_cols, split_rows, P(None), P(None), P(None))
    out_specs = (P('dp', None), cache_spec, cache_spec)
    return jax.shard_map(local_layer, mesh=mesh, in_specs=in_specs, out_specs=out_specs, check_vma=False)
```

```python
import math
import jax
import jax.numpy as jnp
from jax import lax
from jax.experimental import pallas as pl
from jax.experimental.pallas import tpu as pltpu
from jax.sharding import PartitionSpec as P

BUCKET_EDGES = tuple(range(1, 16)) + (16,) + tuple(int(math.ceil(16.0 * 8.0 ** (m / 16.0))) for m in range(1, 16))
NEG_FILL = -1e30
MESH = pl.DeviceIdType.MESH
F32 = jnp.float32
BF16 = jnp.bfloat16
K_ORDER = (2, 1, 3)


def rms_norm(values, norm_scale):
    inv_rms = lax.rsqrt(jnp.mean(values * values, axis=-1, keepdims=True) + 1e-6)
    return (values * inv_rms * norm_scale.astype(F32)).astype(BF16)


def gelu_tanh(u):
    return u * (0.5 * (1.0 + jnp.tanh(math.sqrt(2.0 / math.pi) * (u + 0.044715 * (u * u * u)))))


def dot_nt(a, b):
    return lax.dot_general(a, b, (((1,), (1,)), ((), ())), preferred_element_type=F32)


def dot_nn(a, b):
    return jnp.dot(a, b, preferred_element_type=F32)


def tail_kernel(x_hbm, attn_ref, mask_ref, ck_hbm, cv_hbm, wo_hbm, cq_hbm, co_hbm, wg_hbm, wu_hbm, wd_hbm, nc_ref, nm_ref,
                out_ref,
                x_buf, ck, cv, wo2, cq2, co2, wg2, wu2, wd2, att_in, pair, q_snd, q_all, o_snd, o_rcv, scores,
                y_snd, y_rcv, own, z_snd, z_rcv, h_buf, act,
                loc_sem, w_ssem, w_rsem, ys_sem, yr_sem, zs_sem, zr_sem, gys_sem, gyr_sem, gzs_sem, gzr_sem, cs_sem, cr_sem):
    me = lax.axis_index("tp")
    c = lax.rem(me, 2)
    y = lax.rem(me // 2, 2)
    z = me // 4
    core_peer = {"tp": z * 4 + y * 2 + (1 - c)}
    y_peer = {"tp": z * 4 + (1 - y) * 2 + c}
    z_peer = {k: {"tp": lax.rem(z + k, 4) * 4 + y * 2 + c} for k in (1, 2, 3)}
    my_row = c * 256 + y * 128 + z * 32
    sends = []

    def remote(src, dst, ssem, rsem, peer):
        return pltpu.make_async_remote_copy(src_ref=src, dst_ref=dst, send_sem=ssem, recv_sem=rsem, device_id=peer, device_id_type=MESH)

    def start(src, dst, ssem, rsem, peer):
        copy = remote(src, dst, ssem, rsem, peer)
        copy.start()
        sends.append(copy)
        return copy

    def chunk(base, zz):
        return pl.ds(pl.multiple_of(base + zz * 32, 32), 32)

    half = wg2.shape[0] // 2
    local = [
        pltpu.make_async_copy(x_hbm.at[pl.ds(pl.multiple_of(my_row, 32), 32)], x_buf, loc_sem.at[0]),
        pltpu.make_async_copy(wo_hbm, wo2.at[pl.ds(0, 64)], loc_sem.at[1]),
        pltpu.make_async_copy(cq_hbm, cq2.at[0], loc_sem.at[2]),
        pltpu.make_async_copy(ck_hbm, ck, loc_sem.at[3]),
        pltpu.make_async_copy(cv_hbm, cv, loc_sem.at[4]),
        pltpu.make_async_copy(co_hbm, co2.at[pl.ds(0, 64)], loc_sem.at[5]),
        pltpu.make_async_copy(wg_hbm, wg2.at[pl.ds(0, half)], loc_sem.at[6]),
        pltpu.make_async_copy(wu_hbm, wu2.at[pl.ds(0, half)], loc_sem.at[7]),
        pltpu.make_async_copy(wd_hbm, wd2.at[pl.ds(0, half)], loc_sem.at[8]),
    ]
    for copy in local:
        copy.start()

    barrier = pltpu.get_barrier_semaphore()
    for peer in (core_peer, y_peer, z_peer[1], z_peer[2], z_peer[3]):
        pl.semaphore_signal(barrier, inc=1, device_id=peer, device_id_type=MESH)
    pl.semaphore_wait(barrier, 5)

    att_copy = start(attn_ref.at[pl.ds(pl.multiple_of((1 - c) * 256, 256), 256)], att_in, w_ssem.at[0], w_rsem.at[0], core_peer)
    wo_copy = start(wo_hbm, wo2.at[pl.ds(64, 64)], w_ssem.at[1], w_rsem.at[1], core_peer)
    cq_copy = start(cq_hbm, cq2.at[1], w_ssem.at[2], w_rsem.at[2], core_peer)
    co_copy = start(co_hbm, co2.at[pl.ds(64, 64)], w_ssem.at[3], w_rsem.at[3], core_peer)
    wg_copy = start(wg_hbm, wg2.at[pl.ds(half, half)], w_ssem.at[4], w_rsem.at[4], core_peer)
    wu_copy = start(wu_hbm, wu2.at[pl.ds(half, half)], w_ssem.at[5], w_rsem.at[5], core_peer)
    wd_copy = start(wd_hbm, wd2.at[pl.ds(half, half)], w_ssem.at[6], w_rsem.at[6], core_peer)

    def reduce_scatter(p, partial_of):
        y_snd[p] = partial_of((1 - y) * 128).astype(BF16)
        y_copies = {}
        for k in K_ORDER + (0,):
            zz = lax.rem(z + k, 4)
            y_copies[k] = start(y_snd.at[p, chunk(0, zz)], y_rcv.at[p, k], ys_sem.at[p, k], yr_sem.at[p, k], y_peer)
        own[...] = partial_of(y * 128)
        z_copies = {}
        for k in K_ORDER:
            zz = lax.rem(z + k, 4)
            y_copies[k].wait_recv()
            z_snd[p, k - 1] = (own[chunk(0, zz)] + y_rcv[p, k].astype(F32)).astype(BF16)
            z_copies[k] = start(z_snd.at[p, k - 1], z_rcv.at[p, k - 1], zs_sem.at[p, k - 1], zr_sem.at[p, k - 1], z_peer[k])
        y_copies[0].wait_recv()
        total = own[chunk(0, z)] + y_rcv[p, 0].astype(F32)
        for k in (1, 3, 2):
            z_copies[k].wait_recv()
            total = total + z_rcv[p, k - 1].astype(F32)
        return total

    def gather(p, buf, base):
        mine = buf.at[chunk(base + y * 128, z)]
        start(mine, mine, gys_sem.at[p, 0], gyr_sem.at[p, 0], y_peer)
        for k in K_ORDER:
            start(mine, mine, gzs_sem.at[p, k - 1], gzr_sem.at[p, k - 1], z_peer[k])

    def gathered_z(p, buf, base, k):
        part = buf.at[chunk(base + y * 128, lax.rem(z + 4 - k, 4))]
        remote(part, part, gzs_sem.at[p, k - 1], gzr_sem.at[p, k - 1], z_peer[k]).wait_recv()
        start(part, part, gys_sem.at[p, k], gyr_sem.at[p, k], y_peer)
        return part

    def gathered_y(p, buf, base, k):
        part = buf.at[chunk(base + (1 - y) * 128, lax.rem(z + 4 - k, 4))]
        remote(part, part, gys_sem.at[p, k], gyr_sem.at[p, k], y_peer).wait_recv()
        return part

    pair[:, 0:64] = attn_ref[pl.ds(pl.multiple_of(c * 256, 256), 256), :]
    att_copy.wait_recv()
    pair[:, 64:128] = att_in[...]
    local[1].wait()
    wo_copy.wait_recv()

    def rows_of(base):
        return pl.ds(pl.multiple_of(base, 128), 128)

    total = reduce_scatter(0, lambda base: dot_nn(pair[rows_of(base)], wo2[...]))
    local[0].wait()
    resid = x_buf[...].astype(F32) + total
    h_buf[0, chunk(y * 128, z)] = rms_norm(resid, nc_ref[...])
    gather(0, h_buf.at[0], 0)
    for k in (1, 3, 2):
        gathered_z(0, h_buf.at[0], 0, k)
    for k in (0, 1, 3, 2):
        gathered_y(0, h_buf.at[0], 0, k)

    cq_copy.wait_recv()
    q_snd[...] = dot_nt(cq2[1], h_buf[0]).astype(BF16)
    q_copy = start(q_snd, q_all.at[c], w_ssem.at[7], w_rsem.at[7], core_peer)
    local[2].wait()
    q_all[c] = dot_nt(cq2[0], h_buf[0]).astype(BF16)
    local[3].wait()
    local[4].wait()

    def cross(half_id):
        outs = []
        for block in range(2):
            lanes = pl.ds(pl.multiple_of(half_id * 256 + block * 128, 128), 128)
            q_blk = q_all[half_id, :, block * 128:block * 128 + 128].astype(F32)

            def score_step(i, carry):
                rows = pl.ds(pl.multiple_of(i * 8, 8), 8)
                scores[rows, :] = jnp.sum(ck[rows, :, lanes].astype(F32) * q_blk[None], axis=1)
                return carry

            lax.fori_loop(0, 8, score_step, 0)
            s = scores[...] + jnp.where(mask_ref[:, lanes] != 0, 0.0, NEG_FILL)
            e = jnp.exp(s - jnp.max(s, axis=0, keepdims=True))
            scores[...] = (e / jnp.sum(e, axis=0, keepdims=True)).astype(BF16).astype(F32)

            def mix_step(i, acc):
                rows = pl.ds(pl.multiple_of(i * 8, 8), 8)
                p_blk = scores[rows, :]
                for j in range(8):
                    acc = acc + cv[i * 8 + j, :, lanes].astype(F32) * p_blk[j:j + 1, :]
                return acc

            outs.append(lax.fori_loop(0, 8, mix_step, jnp.zeros((64, 128), F32)).astype(BF16))
        return outs

    mine = cross(c)
    q_in = remote(q_snd, q_all.at[1 - c], w_ssem.at[7], w_rsem.at[7], core_peer)
    q_in.wait_recv()
    theirs = cross(1 - c)
    for block in range(2):
        o_snd[:, block * 128:block * 128 + 128] = theirs[block]
    o_copy = start(o_snd, o_rcv, w_ssem.at[8], w_rsem.at[8], core_peer)
    for block in range(2):
        pair[block * 128:block * 128 + 128, 0:64] = mine[block].astype(F32).T.astype(BF16)
    o_copy.wait_recv()
    pair[:, 64:128] = o_rcv[...].astype(F32).T.astype(BF16)
    local[5].wait()
    co_copy.wait_recv()
    resid = resid + reduce_scatter(1, lambda base: dot_nn(pair[rows_of(base)], co2[...]))
    h_buf[1, chunk(y * 128, z)] = rms_norm(resid, nm_ref[...])
    gather(1, h_buf.at[1], 0)
    for copy in local[6:]:
        copy.wait()
    for copy in (wg_copy, wu_copy, wd_copy):
        copy.wait_recv()
    for k in (1, 3, 2):
        gathered_z(1, h_buf.at[1], 0, k)

    def mlp(base):
        h = h_buf[1, rows_of(base)]
        act[rows_of(base)] = (gelu_tanh(dot_nt(h, wg2[...])) * dot_nt(h, wu2[...])).astype(BF16)

    mlp(y * 128)
    for k in (0, 1, 3, 2):
        gathered_y(1, h_buf.at[1], 0, k)
    mlp((1 - y) * 128)
    resid = resid + reduce_scatter(2, lambda base: dot_nn(act[rows_of(base)], wd2[...]))

    out_ref[pl.ds(pl.multiple_of(my_row, 32), 32)] = resid.astype(BF16)
    gather(2, out_ref, c * 256)
    parts = [out_ref.at[chunk(c * 256 + y * 128, z)]]

    def to_core(part, slot):
        start(part, part, cs_sem.at[slot], cr_sem.at[slot], core_peer)

    to_core(parts[0], 0)
    for k in (1, 3, 2):
        to_core(gathered_z(2, out_ref, c * 256, k), k)
    for k in (0, 1, 3, 2):
        to_core(gathered_y(2, out_ref, c * 256, k), 4 + k)
    for yy in range(2):
        for k in range(4):
            base = (1 - c) * 256 + (y if yy == 0 else 1 - y) * 128
            part = out_ref.at[chunk(base, lax.rem(z + 4 - k, 4))]
            remote(part, part, cs_sem.at[yy * 4 + k], cr_sem.at[yy * 4 + k], core_peer).wait_recv()
    for copy in sends:
        copy.wait_send()


def tail(x_in, attn, mask_t, ck_t, cv_t, wo, cq_t, co, wg_t, wu_t, wd, nc, nm):
    hbm = pl.BlockSpec(memory_space=pltpu.HBM)
    vmem = pl.BlockSpec(memory_space=pltpu.VMEM)
    units = wd.shape[0]
    dma = pltpu.SemaphoreType.DMA
    scratch = [
        pltpu.VMEM((32, 1024), BF16), pltpu.VMEM(ck_t.shape, BF16), pltpu.VMEM(cv_t.shape, BF16),
        pltpu.VMEM((128, 1024), BF16), pltpu.VMEM((2, 64, 1024), BF16), pltpu.VMEM((128, 1024), BF16),
        pltpu.VMEM((2 * units, 1024), BF16), pltpu.VMEM((2 * units, 1024), BF16), pltpu.VMEM((2 * units, 1024), BF16),
        pltpu.VMEM((256, 64), BF16), pltpu.VMEM((256, 128), BF16), pltpu.VMEM((64, 256), BF16), pltpu.VMEM((2, 64, 256), BF16),
        pltpu.VMEM((64, 256), BF16), pltpu.VMEM((64, 256), BF16), pltpu.VMEM((64, 128), F32),
        pltpu.VMEM((3, 128, 1024), BF16), pltpu.VMEM((3, 4, 32, 1024), BF16), pltpu.VMEM((128, 1024), F32),
        pltpu.VMEM((3, 3, 32, 1024), BF16), pltpu.VMEM((3, 3, 32, 1024), BF16), pltpu.VMEM((2, 256, 1024), BF16),
        pltpu.VMEM((256, 2 * units), BF16),
        dma((9,)), dma((9,)), dma((9,)), dma((3, 4)), dma((3, 4)), dma((3, 3)), dma((3, 3)),
        dma((3, 4)), dma((3, 4)), dma((3, 3)), dma((3, 3)), dma((8,)), dma((8,)),
    ]
    return pl.pallas_call(
        tail_kernel,
        out_shape=jax.ShapeDtypeStruct(x_in.shape, BF16),
        in_specs=[hbm, vmem, vmem] + [hbm] * 8 + [vmem, vmem],
        out_specs=vmem,
        scratch_shapes=scratch,
        compiler_params=pltpu.CompilerParams(collective_id=0, has_side_effects=True, vmem_limit_bytes=60 * 1024 * 1024),
        name="tail",
    )(x_in, attn, mask_t, ck_t, cv_t, wo, cq_t, co, wg_t, wu_t, wd, nc, nm)


def head_kernel(tok_ref, rb_ref, x_ref, wq_ref, wk_ref, wv_ref, ns_ref, k_hbm, v_hbm,
                attn_ref, nk_hbm, nv_hbm,
                kbuf, vbuf, h_buf, qq, k_new, v_new, table, in_sem, out_sem):
    rows, depth, t_len = kbuf.shape
    n_chunks = in_sem.shape[1]
    size = rows // n_chunks

    def chunk_copy(i, which):
        hbm, buf = ((k_hbm, kbuf), (v_hbm, vbuf))[which]
        part = pl.ds(i * size, size)
        return pltpu.make_async_copy(hbm.at[part], buf.at[part], in_sem.at[which, i])

    def chunk_out(i, which):
        hbm, buf = ((nk_hbm, kbuf), (nv_hbm, vbuf))[which]
        part = pl.ds(i * size, size)
        return pltpu.make_async_copy(buf.at[part], hbm.at[part], out_sem.at[which, i])

    for i in range(n_chunks):
        chunk_copy(i, 0).start()
        chunk_copy(i, 1).start()

    distance = lax.broadcasted_iota(jnp.int32, (t_len, t_len), 0) - lax.broadcasted_iota(jnp.int32, (t_len, t_len), 1)
    bias = jnp.full((t_len, t_len), rb_ref[0], F32)
    for bucket, edge in enumerate(BUCKET_EDGES):
        bias = jnp.where(distance >= edge, rb_ref[bucket + 1], bias)
    table[...] = jnp.where(distance >= 0, bias, NEG_FILL)

    wqq = jnp.concatenate([wq_ref[...], wq_ref[...]], axis=0)
    for i in range(rows // 128):
        part = slice(i * 128, i * 128 + 128)
        h = rms_norm(x_ref[part, :].astype(F32), ns_ref[...])
        qq[part, :] = dot_nt(h, wqq).astype(BF16).astype(F32)
        k_new[i] = dot_nt(wk_ref[...], h).astype(BF16).astype(F32)
        v_new[i] = dot_nt(wv_ref[...], h).astype(BF16).astype(F32)

    lane = lax.broadcasted_iota(jnp.int32, (depth, t_len), 1)
    row8 = lax.broadcasted_iota(jnp.int32, (8, 128), 0)
    half8 = lax.broadcasted_iota(jnp.int32, (8, 128), 1) // depth

    def step(i, carry):
        chunk_copy(i, 0).wait()
        chunk_copy(i, 1).wait()
        shift = lax.rem(i, 2) * size
        k_cols = pltpu.roll(k_new[i // 2], shift, 1)
        v_cols = pltpu.roll(v_new[i // 2], shift, 1)
        scores = []
        for g in range(size // 8):
            k8, bias8 = [], []
            for j in range(8):
                b = i * size + g * 8 + j
                pos = tok_ref[b]
                at_pos = lane == pos
                col = g * 8 + j
                k_b = jnp.where(at_pos, jnp.broadcast_to(k_cols[:, col:col + 1], (depth, t_len)), kbuf[b].astype(F32)).astype(BF16)
                v_b = jnp.where(at_pos, jnp.broadcast_to(v_cols[:, col:col + 1], (depth, t_len)), vbuf[b].astype(F32)).astype(BF16)
                kbuf[b] = k_b
                vbuf[b] = v_b
                k8.append(k_b)
                bias8.append(table[pl.ds(pos, 1), :])
            q8 = qq[pl.ds(pl.multiple_of(i * size + g * 8, 8), 8), :]
            q_diag = jnp.concatenate([jnp.where(row8 == 2 * m + half8, q8, 0.0) for m in range(4)], axis=1).astype(BF16)
            scores.append(dot_nn(q_diag, jnp.concatenate(k8, axis=0)) + jnp.concatenate(bias8, axis=0))
        chunk_out(i, 0).start()
        chunk_out(i, 1).start()
        s = jnp.concatenate(scores, axis=0)
        e = jnp.exp(s - jnp.max(s, axis=1, keepdims=True))
        p = (e / jnp.sum(e, axis=1, keepdims=True)).astype(BF16).astype(F32)
        outs = []
        for g in range(size // 8):
            p8 = p[g * 8:g * 8 + 8, :]
            p_diag = jnp.concatenate([jnp.where(row8 == j, p8, 0.0) for j in range(8)], axis=1).astype(BF16)
            v8 = jnp.concatenate([vbuf[i * size + g * 8 + j] for j in range(8)], axis=1)
            outs.append(dot_nt(p_diag, v8))
        attn_ref[pl.ds(pl.multiple_of(i * size, size), size), :] = jnp.concatenate(outs, axis=0).astype(BF16)
        return carry

    lax.fori_loop(0, n_chunks, step, 0)
    for i in range(n_chunks):
        chunk_out(i, 0).wait()
        chunk_out(i, 1).wait()


def head(tok_pos, rel_bias, x_in, wq_t, wk_t, wv_t, ns, k_t, v_t):
    hbm = pl.BlockSpec(memory_space=pltpu.HBM)
    vmem = pl.BlockSpec(memory_space=pltpu.VMEM)
    smem = pl.BlockSpec(memory_space=pltpu.SMEM)
    rows, depth, t_len = k_t.shape
    dma = pltpu.SemaphoreType.DMA
    n_chunks = 8
    return pl.pallas_call(
        head_kernel,
        out_shape=(jax.ShapeDtypeStruct((rows, depth), BF16), jax.ShapeDtypeStruct(k_t.shape, BF16), jax.ShapeDtypeStruct(v_t.shape, BF16)),
        in_specs=[smem, smem] + [vmem] * 5 + [hbm] * 2,
        out_specs=(vmem, hbm, hbm),
        scratch_shapes=[
            pltpu.VMEM(k_t.shape, BF16), pltpu.VMEM(v_t.shape, BF16), pltpu.VMEM((8, 128), BF16),
            pltpu.VMEM((rows, 2 * depth), F32), pltpu.VMEM((rows // 128, depth, 128), F32), pltpu.VMEM((rows // 128, depth, 128), F32),
            pltpu.VMEM((t_len, t_len), F32), dma((2, n_chunks)), dma((2, n_chunks)),
        ],
        compiler_params=pltpu.CompilerParams(vmem_limit_bytes=60 * 1024 * 1024),
        name="head",
    )(tok_pos, rel_bias, x_in, wq_t, wk_t, wv_t, ns, k_t, v_t)


def solution(mesh):
    def local_layer(x_in, tok_pos, self_k, self_v, cross_k, cross_v, enc_mask, rel_bias, w_q, w_k, w_v, w_o, cross_q, cross_o, w_gate, w_up, w_down, norm_self, norm_cross, norm_mlp):
        k_t = jnp.transpose(self_k[:, :, 0, :], (0, 2, 1))
        v_t = jnp.transpose(self_v[:, :, 0, :], (0, 2, 1))
        attn, new_k, new_v = head(tok_pos, rel_bias[:, 0], x_in, w_q.T, w_k.T, w_v.T, norm_self[None, :], k_t, v_t)
        new_self_k = jnp.transpose(new_k, (0, 2, 1))[:, :, None, :]
        new_self_v = jnp.transpose(new_v, (0, 2, 1))[:, :, None, :]
        ck_t = jnp.transpose(cross_k[:, :, 0, :], (1, 2, 0))
        cv_t = jnp.transpose(cross_v[:, :, 0, :], (1, 2, 0))
        out = tail(x_in, attn, enc_mask.T, ck_t, cv_t, w_o, cross_q.T, cross_o, w_gate.T, w_up.T, w_down,
                   norm_cross[None, :], norm_mlp[None, :])
        return out, new_self_k, new_self_v

    cache_spec = P('dp', None, 'tp', None)
    split_cols = P(None, 'tp')
    split_rows = P('tp', None)
    in_specs = (P('dp', None), P('dp'), cache_spec, cache_spec, cache_spec, cache_spec, P('dp', None), split_cols, split_cols, split_cols, split_cols, split_rows, split_cols, split_rows, split_cols, split_cols, split_rows, P(None), P(None), P(None))
    out_specs = (P('dp', None), cache_spec, cache_spec)
    return jax.shard_map(local_layer, mesh=mesh, in_specs=in_specs, out_specs=out_specs, check_vma=False)
```

```python
import math
import jax
import jax.numpy as jnp
from jax import lax
from jax.experimental import pallas as pl
from jax.experimental.pallas import tpu as pltpu
from jax.sharding import PartitionSpec as P

BUCKET_EDGES = tuple(range(1, 16)) + (16,) + tuple(int(math.ceil(16.0 * 8.0 ** (m / 16.0))) for m in range(1, 16))
NEG_FILL = -1e30
MESH = pl.DeviceIdType.MESH
F32 = jnp.float32
BF16 = jnp.bfloat16
K_ORDER = (2, 1, 3)


def rms_norm(values, norm_scale):
    inv_rms = lax.rsqrt(jnp.mean(values * values, axis=-1, keepdims=True) + 1e-6)
    return (values * inv_rms * norm_scale.astype(F32)[None, :]).astype(BF16)


def gelu_tanh(u):
    return u * (0.5 * (1.0 + jnp.tanh(math.sqrt(2.0 / math.pi) * (u + 0.044715 * (u * u * u)))))


def dot_nt(a, b):
    return lax.dot_general(a, b, (((1,), (1,)), ((), ())), preferred_element_type=F32)


def dot_nn(a, b):
    return jnp.dot(a, b, preferred_element_type=F32)


def tail_kernel(x_hbm, attn_ref, mask_ref, ck_hbm, cv_hbm, wo_hbm, cq_hbm, co_hbm, wg_hbm, wu_hbm, wd_hbm, nc_ref, nm_ref,
                out_ref,
                x_buf, ck, cv, wo2, cq2, co2, wg2, wu2, wd2, att_in, pair, q_snd, q_all, o_snd, o_rcv, scores,
                y_snd, y_rcv, own, z_snd, z_rcv, h_buf, act,
                loc_sem, w_ssem, w_rsem, ys_sem, yr_sem, zs_sem, zr_sem, gys_sem, gyr_sem, gzs_sem, gzr_sem, cs_sem, cr_sem):
    me = lax.axis_index("tp")
    c = lax.rem(me, 2)
    y = lax.rem(me // 2, 2)
    z = me // 4
    core_peer = {"tp": z * 4 + y * 2 + (1 - c)}
    y_peer = {"tp": z * 4 + (1 - y) * 2 + c}
    z_peer = {k: {"tp": lax.rem(z + k, 4) * 4 + y * 2 + c} for k in (1, 2, 3)}
    sends = []

    def remote(src, dst, ssem, rsem, peer):
        return pltpu.make_async_remote_copy(src_ref=src, dst_ref=dst, send_sem=ssem, recv_sem=rsem, device_id=peer, device_id_type=MESH)

    def start(src, dst, ssem, rsem, peer):
        copy = remote(src, dst, ssem, rsem, peer)
        copy.start()
        sends.append(copy)
        return copy

    def span(base, size):
        return pl.ds(pl.multiple_of(base, size), size)

    def chunk(base, zz):
        return span(base + zz * 16, 16)

    half = wg2.shape[0] // 2
    local = [
        pltpu.make_async_copy(x_hbm.at[chunk(c * 256 + y * 64, z)], x_buf.at[0], loc_sem.at[0]),
        pltpu.make_async_copy(x_hbm.at[chunk(c * 256 + 128 + y * 64, z)], x_buf.at[1], loc_sem.at[1]),
        pltpu.make_async_copy(wo_hbm, wo2.at[pl.ds(0, 64)], loc_sem.at[2]),
        pltpu.make_async_copy(cq_hbm, cq2.at[0], loc_sem.at[3]),
        pltpu.make_async_copy(ck_hbm, ck, loc_sem.at[4]),
        pltpu.make_async_copy(cv_hbm, cv, loc_sem.at[5]),
        pltpu.make_async_copy(co_hbm, co2.at[pl.ds(0, 64)], loc_sem.at[6]),
        pltpu.make_async_copy(wg_hbm, wg2.at[pl.ds(0, half)], loc_sem.at[7]),
        pltpu.make_async_copy(wu_hbm, wu2.at[pl.ds(0, half)], loc_sem.at[8]),
        pltpu.make_async_copy(wd_hbm, wd2.at[pl.ds(0, half)], loc_sem.at[9]),
    ]
    for copy in local:
        copy.start()

    barrier = pltpu.get_barrier_semaphore()
    for peer in (core_peer, y_peer, z_peer[1], z_peer[2], z_peer[3]):
        pl.semaphore_signal(barrier, inc=1, device_id=peer, device_id_type=MESH)
    pl.semaphore_wait(barrier, 5)

    att_copy = start(attn_ref.at[span((1 - c) * 256, 256)], att_in, w_ssem.at[0], w_rsem.at[0], core_peer)
    wo_copy = start(wo_hbm, wo2.at[pl.ds(64, 64)], w_ssem.at[1], w_rsem.at[1], core_peer)
    cq_copy = start(cq_hbm, cq2.at[1], w_ssem.at[2], w_rsem.at[2], core_peer)
    co_copy = start(co_hbm, co2.at[pl.ds(64, 64)], w_ssem.at[3], w_rsem.at[3], core_peer)
    wg_copy = start(wg_hbm, wg2.at[pl.ds(half, half)], w_ssem.at[4], w_rsem.at[4], core_peer)
    wu_copy = start(wu_hbm, wu2.at[pl.ds(half, half)], w_ssem.at[5], w_rsem.at[5], core_peer)
    wd_copy = start(wd_hbm, wd2.at[pl.ds(half, half)], w_ssem.at[6], w_rsem.at[6], core_peer)
    waited = set()

    def once(name, *waits):
        if name not in waited:
            waited.add(name)
            for wait in waits:
                wait()

    def reduce_scatter(p, b, partial_of):
        y_snd[p, b] = partial_of((1 - y) * 64).astype(BF16)
        y_copies = {}
        for k in K_ORDER + (0,):
            y_copies[k] = start(y_snd.at[p, b, chunk(0, lax.rem(z + k, 4))], y_rcv.at[p, b, k], ys_sem.at[p, b, k], yr_sem.at[p, b, k], y_peer)
        own[b] = partial_of(y * 64)
        yield
        z_copies = {}
        for k in K_ORDER:
            y_copies[k].wait_recv()
            z_snd[p, b, k - 1] = (own[b, chunk(0, lax.rem(z + k, 4))] + y_rcv[p, b, k].astype(F32)).astype(BF16)
            z_copies[k] = start(z_snd.at[p, b, k - 1], z_rcv.at[p, b, k - 1], zs_sem.at[p, b, k - 1], zr_sem.at[p, b, k - 1], z_peer[k])
        yield
        y_copies[0].wait_recv()
        total = own[b, chunk(0, z)] + y_rcv[p, b, 0].astype(F32)
        for k in (1, 3, 2):
            z_copies[k].wait_recv()
            total = total + z_rcv[p, b, k - 1].astype(F32)
        return total

    def gather(p, b, buf, base, on_part=None):
        def part_at(yy, k):
            return buf.at[chunk(base + yy * 64, lax.rem(z + 4 - k, 4))]

        def done(part, slot):
            if on_part is not None:
                on_part(part, slot)

        mine = part_at(y, 0)
        start(mine, mine, gys_sem.at[p, b, 0], gyr_sem.at[p, b, 0], y_peer)
        for k in K_ORDER:
            start(mine, mine, gzs_sem.at[p, b, k - 1], gzr_sem.at[p, b, k - 1], z_peer[k])
        done(mine, 0)
        yield
        for k in (1, 3, 2):
            part = part_at(y, k)
            remote(part, part, gzs_sem.at[p, b, k - 1], gzr_sem.at[p, b, k - 1], z_peer[k]).wait_recv()
            start(part, part, gys_sem.at[p, b, k], gyr_sem.at[p, b, k], y_peer)
            done(part, k)
        yield
        for k in (0, 1, 3, 2):
            part = part_at(1 - y, k)
            remote(part, part, gys_sem.at[p, b, k], gyr_sem.at[p, b, k], y_peer).wait_recv()
            done(part, 4 + k)

    def cross(half_id, b):
        lanes = span(half_id * 256 + b * 128, 128)
        q_blk = q_all[half_id, b].astype(F32)

        def score_step(i, carry):
            rows = span(i * 8, 8)
            scores[rows, :] = jnp.sum(ck[rows, :, lanes].astype(F32) * q_blk[None], axis=1)
            return carry

        lax.fori_loop(0, 8, score_step, 0)
        s = scores[...] + jnp.where(mask_ref[:, lanes] != 0, 0.0, NEG_FILL)
        e = jnp.exp(s - jnp.max(s, axis=0, keepdims=True))
        scores[...] = (e / jnp.sum(e, axis=0, keepdims=True)).astype(BF16).astype(F32)

        def mix_step(i, acc):
            p_blk = scores[span(i * 8, 8), :]
            for j in range(8):
                acc = acc + cv[i * 8 + j, :, lanes].astype(F32) * p_blk[j:j + 1, :]
            return acc

        return lax.fori_loop(0, 8, mix_step, jnp.zeros((64, 128), F32)).astype(BF16)

    def flow(b):
        once("att", att_copy.wait_recv, local[2].wait, wo_copy.wait_recv)
        pair[b, :, 0:64] = attn_ref[span(c * 256 + b * 128, 128), :]
        pair[b, :, 64:128] = att_in[b * 128:b * 128 + 128, :]
        total = yield from reduce_scatter(0, b, lambda base: dot_nn(pair[b, span(base, 64)], wo2[...]))
        local[b].wait()
        resid = x_buf[b].astype(F32) + total
        h_buf[0, b, chunk(y * 64, z)] = rms_norm(resid, nc_ref[...])
        yield from gather(0, b, h_buf.at[0, b], 0)
        once("cq", cq_copy.wait_recv, local[3].wait, local[4].wait, local[5].wait)
        q_snd[b] = dot_nt(cq2[1], h_buf[0, b]).astype(BF16)
        q_copy = start(q_snd.at[b], q_all.at[c, b], w_ssem.at[7 + b], w_rsem.at[7 + b], core_peer)
        q_all[c, b] = dot_nt(cq2[0], h_buf[0, b]).astype(BF16)
        mine = cross(c, b)
        pair[b, :, 0:64] = mine.astype(F32).T.astype(BF16)
        remote(q_snd.at[b], q_all.at[1 - c, b], w_ssem.at[7 + b], w_rsem.at[7 + b], core_peer).wait_recv()
        o_snd[b] = cross(1 - c, b)
        o_copy = start(o_snd.at[b], o_rcv.at[b], w_ssem.at[9 + b], w_rsem.at[9 + b], core_peer)
        yield
        o_copy.wait_recv()
        pair[b, :, 64:128] = o_rcv[b].astype(F32).T.astype(BF16)
        once("co", local[6].wait, co_copy.wait_recv)
        total = yield from reduce_scatter(1, b, lambda base: dot_nn(pair[b, span(base, 64)], co2[...]))
        resid = resid + total
        h_buf[1, b, chunk(y * 64, z)] = rms_norm(resid, nm_ref[...])
        yield from gather(1, b, h_buf.at[1, b], 0)
        once("mlp", local[7].wait, local[8].wait, local[9].wait, wg_copy.wait_recv, wu_copy.wait_recv, wd_copy.wait_recv)
        h = h_buf[1, b]
        act[b] = (gelu_tanh(dot_nt(h, wg2[...])) * dot_nt(h, wu2[...])).astype(BF16)
        total = yield from reduce_scatter(2, b, lambda base: dot_nn(act[b, span(base, 64)], wd2[...]))
        resid = resid + total
        first = c * 256 + b * 128
        out_ref[chunk(first + y * 64, z)] = resid.astype(BF16)
        yield from gather(2, b, out_ref, first, lambda part, slot: start(part, part, cs_sem.at[b, slot], cr_sem.at[b, slot], core_peer))

    flows = [flow(0), flow(1)]
    while flows:
        for item in list(flows):
            try:
                next(item)
            except StopIteration:
                flows.remove(item)
    for b in range(2):
        for slot in range(8):
            yy = y if slot < 4 else 1 - y
            part = out_ref.at[chunk((1 - c) * 256 + b * 128 + yy * 64, lax.rem(z + 4 - slot % 4, 4))]
            remote(part, part, cs_sem.at[b, slot], cr_sem.at[b, slot], core_peer).wait_recv()
    for copy in sends:
        copy.wait_send()


def tail(x_in, attn, mask_t, ck_t, cv_t, wo, cq_t, co, wg_t, wu_t, wd, nc, nm):
    hbm = pl.BlockSpec(memory_space=pltpu.HBM)
    vmem = pl.BlockSpec(memory_space=pltpu.VMEM)
    units = wd.shape[0]
    dma = pltpu.SemaphoreType.DMA
    scratch = [
        pltpu.VMEM((2, 16, 1024), BF16), pltpu.VMEM(ck_t.shape, BF16), pltpu.VMEM(cv_t.shape, BF16),
        pltpu.VMEM((128, 1024), BF16), pltpu.VMEM((2, 64, 1024), BF16), pltpu.VMEM((128, 1024), BF16),
        pltpu.VMEM((2 * units, 1024), BF16), pltpu.VMEM((2 * units, 1024), BF16), pltpu.VMEM((2 * units, 1024), BF16),
        pltpu.VMEM((256, 64), BF16), pltpu.VMEM((2, 128, 128), BF16), pltpu.VMEM((2, 64, 128), BF16), pltpu.VMEM((2, 2, 64, 128), BF16),
        pltpu.VMEM((2, 64, 128), BF16), pltpu.VMEM((2, 64, 128), BF16), pltpu.VMEM((64, 128), F32),
        pltpu.VMEM((3, 2, 64, 1024), BF16), pltpu.VMEM((3, 2, 4, 16, 1024), BF16), pltpu.VMEM((2, 64, 1024), F32),
        pltpu.VMEM((3, 2, 3, 16, 1024), BF16), pltpu.VMEM((3, 2, 3, 16, 1024), BF16), pltpu.VMEM((2, 2, 128, 1024), BF16),
        pltpu.VMEM((2, 128, 2 * units), BF16),
        dma((10,)), dma((11,)), dma((11,)), dma((3, 2, 4)), dma((3, 2, 4)), dma((3, 2, 3)), dma((3, 2, 3)),
        dma((3, 2, 4)), dma((3, 2, 4)), dma((3, 2, 3)), dma((3, 2, 3)), dma((2, 8)), dma((2, 8)),
    ]
    return pl.pallas_call(
        tail_kernel,
        out_shape=jax.ShapeDtypeStruct(x_in.shape, BF16),
        in_specs=[hbm, vmem, vmem] + [hbm] * 8 + [vmem, vmem],
        out_specs=vmem,
        scratch_shapes=scratch,
        compiler_params=pltpu.CompilerParams(collective_id=0, has_side_effects=True, vmem_limit_bytes=60 * 1024 * 1024),
        name="tail",
    )(x_in, attn, mask_t, ck_t, cv_t, wo, cq_t, co, wg_t, wu_t, wd, nc, nm)


def head_kernel(tok_ref, rb_ref, x_ref, wq_ref, wk_ref, wv_ref, ns_ref, k_hbm, v_hbm,
                attn_ref, nk_hbm, nv_hbm,
                kbuf, vbuf, h_buf, qq, k_new, v_new, table, in_sem, out_sem):
    rows, depth, t_len = kbuf.shape
    n_chunks = in_sem.shape[1]
    size = rows // n_chunks

    def chunk_copy(i, which):
        hbm, buf = ((k_hbm, kbuf), (v_hbm, vbuf))[which]
        part = pl.ds(i * size, size)
        return pltpu.make_async_copy(hbm.at[part], buf.at[part], in_sem.at[which, i])

    def chunk_out(i, which):
        hbm, buf = ((nk_hbm, kbuf), (nv_hbm, vbuf))[which]
        part = pl.ds(i * size, size)
        return pltpu.make_async_copy(buf.at[part], hbm.at[part], out_sem.at[which, i])

    for i in range(n_chunks):
        chunk_copy(i, 0).start()
        chunk_copy(i, 1).start()

    distance = lax.broadcasted_iota(jnp.int32, (t_len, t_len), 0) - lax.broadcasted_iota(jnp.int32, (t_len, t_len), 1)
    bias = jnp.full((t_len, t_len), rb_ref[0], F32)
    for bucket, edge in enumerate(BUCKET_EDGES):
        bias = jnp.where(distance >= edge, rb_ref[bucket + 1], bias)
    table[...] = jnp.where(distance >= 0, bias, NEG_FILL)

    wqq = jnp.concatenate([wq_ref[...], wq_ref[...]], axis=0)
    for i in range(rows // 128):
        part = slice(i * 128, i * 128 + 128)
        h = rms_norm(x_ref[part, :].astype(F32), ns_ref[...])
        qq[part, :] = dot_nt(h, wqq).astype(BF16).astype(F32)
        k_new[i] = dot_nt(wk_ref[...], h).astype(BF16).astype(F32)
        v_new[i] = dot_nt(wv_ref[...], h).astype(BF16).astype(F32)

    lane = lax.broadcasted_iota(jnp.int32, (depth, t_len), 1)
    row8 = lax.broadcasted_iota(jnp.int32, (8, 128), 0)
    half8 = lax.broadcasted_iota(jnp.int32, (8, 128), 1) // depth

    def step(i, carry):
        chunk_copy(i, 0).wait()
        chunk_copy(i, 1).wait()
        shift = lax.rem(i, 2) * size
        k_cols = pltpu.roll(k_new[i // 2], shift, 1)
        v_cols = pltpu.roll(v_new[i // 2], shift, 1)
        scores = []
        for g in range(size // 8):
            k8, bias8 = [], []
            for j in range(8):
                b = i * size + g * 8 + j
                pos = tok_ref[b]
                at_pos = lane == pos
                col = g * 8 + j
                k_b = jnp.where(at_pos, jnp.broadcast_to(k_cols[:, col:col + 1], (depth, t_len)), kbuf[b].astype(F32)).astype(BF16)
                v_b = jnp.where(at_pos, jnp.broadcast_to(v_cols[:, col:col + 1], (depth, t_len)), vbuf[b].astype(F32)).astype(BF16)
                kbuf[b] = k_b
                vbuf[b] = v_b
                k8.append(k_b)
                bias8.append(table[pl.ds(pos, 1), :])
            q8 = qq[pl.ds(pl.multiple_of(i * size + g * 8, 8), 8), :]
            q_diag = jnp.concatenate([jnp.where(row8 == 2 * m + half8, q8, 0.0) for m in range(4)], axis=1).astype(BF16)
            scores.append(dot_nn(q_diag, jnp.concatenate(k8, axis=0)) + jnp.concatenate(bias8, axis=0))
        chunk_out(i, 0).start()
        chunk_out(i, 1).start()
        s = jnp.concatenate(scores, axis=0)
        e = jnp.exp(s - jnp.max(s, axis=1, keepdims=True))
        p = (e / jnp.sum(e, axis=1, keepdims=True)).astype(BF16).astype(F32)
        outs = []
        for g in range(size // 8):
            p8 = p[g * 8:g * 8 + 8, :]
            p_diag = jnp.concatenate([jnp.where(row8 == j, p8, 0.0) for j in range(8)], axis=1).astype(BF16)
            v8 = jnp.concatenate([vbuf[i * size + g * 8 + j] for j in range(8)], axis=1)
            outs.append(dot_nt(p_diag, v8))
        attn_ref[pl.ds(pl.multiple_of(i * size, size), size), :] = jnp.concatenate(outs, axis=0).astype(BF16)
        return carry

    lax.fori_loop(0, n_chunks, step, 0)
    for i in range(n_chunks):
        chunk_out(i, 0).wait()
        chunk_out(i, 1).wait()


def head(tok_pos, rel_bias, x_in, wq_t, wk_t, wv_t, ns, k_t, v_t):
    hbm = pl.BlockSpec(memory_space=pltpu.HBM)
    vmem = pl.BlockSpec(memory_space=pltpu.VMEM)
    smem = pl.BlockSpec(memory_space=pltpu.SMEM)
    rows, depth, t_len = k_t.shape
    dma = pltpu.SemaphoreType.DMA
    n_chunks = 8
    return pl.pallas_call(
        head_kernel,
        out_shape=(jax.ShapeDtypeStruct((rows, depth), BF16), jax.ShapeDtypeStruct(k_t.shape, BF16), jax.ShapeDtypeStruct(v_t.shape, BF16)),
        in_specs=[smem, smem] + [vmem] * 5 + [hbm] * 2,
        out_specs=(vmem, hbm, hbm),
        scratch_shapes=[
            pltpu.VMEM(k_t.shape, BF16), pltpu.VMEM(v_t.shape, BF16), pltpu.VMEM((8, 128), BF16),
            pltpu.VMEM((rows, 2 * depth), F32), pltpu.VMEM((rows // 128, depth, 128), F32), pltpu.VMEM((rows // 128, depth, 128), F32),
            pltpu.VMEM((t_len, t_len), F32), dma((2, n_chunks)), dma((2, n_chunks)),
        ],
        compiler_params=pltpu.CompilerParams(vmem_limit_bytes=60 * 1024 * 1024),
        name="head",
    )(tok_pos, rel_bias, x_in, wq_t, wk_t, wv_t, ns, k_t, v_t)


def solution(mesh):
    def local_layer(x_in, tok_pos, self_k, self_v, cross_k, cross_v, enc_mask, rel_bias, w_q, w_k, w_v, w_o, cross_q, cross_o, w_gate, w_up, w_down, norm_self, norm_cross, norm_mlp):
        k_t = jnp.transpose(self_k[:, :, 0, :], (0, 2, 1))
        v_t = jnp.transpose(self_v[:, :, 0, :], (0, 2, 1))
        attn, new_k, new_v = head(tok_pos, rel_bias[:, 0], x_in, w_q.T, w_k.T, w_v.T, norm_self, k_t, v_t)
        new_self_k = jnp.transpose(new_k, (0, 2, 1))[:, :, None, :]
        new_self_v = jnp.transpose(new_v, (0, 2, 1))[:, :, None, :]
        ck_t = jnp.transpose(cross_k[:, :, 0, :], (1, 2, 0))
        cv_t = jnp.transpose(cross_v[:, :, 0, :], (1, 2, 0))
        out = tail(x_in, attn, enc_mask.T, ck_t, cv_t, w_o, cross_q.T, cross_o, w_gate.T, w_up.T, w_down,
                   norm_cross, norm_mlp)
        return out, new_self_k, new_self_v

    cache_spec = P('dp', None, 'tp', None)
    split_cols = P(None, 'tp')
    split_rows = P('tp', None)
    in_specs = (P('dp', None), P('dp'), cache_spec, cache_spec, cache_spec, cache_spec, P('dp', None), split_cols, split_cols, split_cols, split_cols, split_rows, split_cols, split_rows, split_cols, split_cols, split_rows, P(None), P(None), P(None))
    out_specs = (P('dp', None), cache_spec, cache_spec)
    return jax.shard_map(local_layer, mesh=mesh, in_specs=in_specs, out_specs=out_specs, check_vma=False)
```

```python
import math
import jax
import jax.numpy as jnp
from jax import lax
from jax.experimental import pallas as pl
from jax.experimental.pallas import tpu as pltpu
from jax.sharding import PartitionSpec as P

BUCKET_EDGES = tuple(range(1, 16)) + (16,) + tuple(int(math.ceil(16.0 * 8.0 ** (m / 16.0))) for m in range(1, 16))
NEG_FILL = -1e30
MESH = pl.DeviceIdType.MESH
F32 = jnp.float32
BF16 = jnp.bfloat16
K_ORDER = (2, 1, 3)


def rms_norm(values, norm_scale):
    inv_rms = lax.rsqrt(jnp.mean(values * values, axis=-1, keepdims=True) + 1e-6)
    return (values * inv_rms * norm_scale.astype(F32)[None, :]).astype(BF16)


def gelu_tanh(u):
    return u * (0.5 * (1.0 + jnp.tanh(math.sqrt(2.0 / math.pi) * (u + 0.044715 * (u * u * u)))))


def dot_nt(a, b):
    return lax.dot_general(a, b, (((1,), (1,)), ((), ())), preferred_element_type=F32)


def dot_nn(a, b):
    return jnp.dot(a, b, preferred_element_type=F32)


def tail_kernel(x_hbm, attn_ref, mask_ref, ck_hbm, cv_hbm, wo_hbm, cq_hbm, co_hbm, wg_hbm, wu_hbm, wd_hbm, woy_hbm, cqy_hbm, coy_hbm, nc_ref, nm_ref,
                out_ref,
                x_buf, ck, cv, wo4, cq4, co4, wg4, wu4, wd4, att_rcv, heads, q_snd, q_rcv, o_buf, o_rcv, scores,
                own, z_snd, z_rcv, h_buf, act,
                loc_sem, w_ssem, w_rsem, at_ssem, at_rsem, q_ssem, q_rsem, o_ssem, o_rsem, zs_sem, zr_sem, gzs_sem, gzr_sem, gys_sem, gyr_sem, cs_sem, cr_sem):
    me = lax.axis_index("tp")
    c = lax.rem(me, 2)
    y = lax.rem(me // 2, 2)
    z = me // 4
    quad = {r: {"tp": z * 4 + (y if r < 2 else 1 - y) * 2 + (c if r == 2 else 1 - c)} for r in (1, 2, 3)}
    quad_c = {0: c, 1: 1 - c, 2: c, 3: 1 - c}
    quad_y = {0: y, 1: y, 2: 1 - y, 3: 1 - y}
    z_peer = {k: {"tp": lax.rem(z + k, 4) * 4 + y * 2 + c} for k in (1, 2, 3)}
    sends = []

    def remote(src, dst, ssem, rsem, peer):
        return pltpu.make_async_remote_copy(src_ref=src, dst_ref=dst, send_sem=ssem, recv_sem=rsem, device_id=peer, device_id_type=MESH)

    def start(src, dst, ssem, rsem, peer):
        copy = remote(src, dst, ssem, rsem, peer)
        copy.start()
        sends.append(copy)
        return copy

    def span(base, size):
        return pl.ds(pl.multiple_of(base, size), size)

    def chunk(base, zz):
        return span(base + zz * 16, 16)

    def slot(ref, r):
        size = ref.shape[0] // 4
        return ref.at[pl.ds(r * size, size)]

    local = [pltpu.make_async_copy(src, dst, loc_sem.at[i]) for i, (src, dst) in enumerate((
        (x_hbm.at[chunk(c * 256 + y * 64, z)], x_buf.at[0]),
        (x_hbm.at[chunk(c * 256 + 128 + y * 64, z)], x_buf.at[1]),
        (wo_hbm, slot(wo4, 0)), (woy_hbm, slot(wo4, 2)),
        (cq_hbm, slot(cq4, 0)), (cqy_hbm, slot(cq4, 2)),
        (ck_hbm, ck), (cv_hbm, cv),
        (co_hbm, slot(co4, 0)), (coy_hbm, slot(co4, 2)),
        (wg_hbm, slot(wg4, 0)), (wu_hbm, slot(wu4, 0)), (wd_hbm, slot(wd4, 0)),
    ))]
    for copy in local:
        copy.start()

    barrier = pltpu.get_barrier_semaphore()
    for peer in (quad[1], quad[2], quad[3], z_peer[1], z_peer[2], z_peer[3]):
        pl.semaphore_signal(barrier, inc=1, device_id=peer, device_id_type=MESH)
    pl.semaphore_wait(barrier, 6)

    def rows_of(b, r):
        return span(quad_c[r] * 256 + b * 128 + quad_y[r] * 64, 64)

    att = {}
    for b in range(2):
        for r in (3, 2, 1):
            att[b, r] = start(attn_ref.at[rows_of(b, r)], att_rcv.at[b, r - 1], at_ssem.at[b, r - 1], at_rsem.at[b, r - 1], quad[r])
    to_core = {}
    for i, (src, dst, r) in enumerate((
        (wo_hbm, wo4, 1), (woy_hbm, wo4, 3), (cq_hbm, cq4, 1), (cqy_hbm, cq4, 3), (co_hbm, co4, 1), (coy_hbm, co4, 3),
        (wg_hbm, wg4, 1), (wu_hbm, wu4, 1), (wd_hbm, wd4, 1),
    )):
        to_core[i] = start(src, slot(dst, r), w_ssem.at[i], w_rsem.at[i], quad[1])
    wg_y = start(wg_hbm, slot(wg4, 2), w_ssem.at[9], w_rsem.at[9], quad[2])
    wu_y = start(wu_hbm, slot(wu4, 2), w_ssem.at[10], w_rsem.at[10], quad[2])
    late = {}

    def start_wd():
        late["wd"] = start(wd_hbm, slot(wd4, 2), w_ssem.at[11], w_rsem.at[11], quad[2])

    def forward_gate_up():
        wg_y.wait_recv()
        late["wg"] = start(slot(wg4, 2), slot(wg4, 3), w_ssem.at[12], w_rsem.at[12], quad[1])
        wu_y.wait_recv()
        late["wu"] = start(slot(wu4, 2), slot(wu4, 3), w_ssem.at[13], w_rsem.at[13], quad[1])

    def forward_wd():
        late["wd"].wait_recv()
        late["wd3"] = start(slot(wd4, 2), slot(wd4, 3), w_ssem.at[14], w_rsem.at[14], quad[1])

    waited = set()

    def once(name, *waits):
        if name not in waited:
            waited.add(name)
            for wait in waits:
                wait()

    def reduce_scatter(p, b, partial):
        own[b] = partial
        z_snd[p, b] = partial.astype(BF16)
        copies = {}
        for k in K_ORDER:
            copies[k] = start(z_snd.at[p, b, chunk(0, lax.rem(z + k, 4))], z_rcv.at[p, b, k - 1], zs_sem.at[p, b, k - 1], zr_sem.at[p, b, k - 1], z_peer[k])
        yield
        total = own[b, chunk(0, z)]
        for k in (1, 3, 2):
            copies[k].wait_recv()
            total = total + z_rcv[p, b, k - 1].astype(F32)
        return total

    def gather_start(p, b, mine):
        for k in K_ORDER:
            start(mine, mine, gzs_sem.at[p, b, k - 1], gzr_sem.at[p, b, k - 1], z_peer[k])

    def gather_wait(p, b, part, k):
        remote(part, part, gzs_sem.at[p, b, k - 1], gzr_sem.at[p, b, k - 1], z_peer[k]).wait_recv()

    def gather(p, b):
        buf = h_buf.at[p, b]
        gather_start(p, b, buf.at[chunk(0, z)])
        yield
        for k in (1, 3, 2):
            gather_wait(p, b, buf.at[chunk(0, lax.rem(z + 4 - k, 4))], k)

    def gather_out(b):
        first = c * 256 + b * 128

        def part_at(yy, k):
            return out_ref.at[chunk(first + yy * 64, lax.rem(z + 4 - k, 4))]

        def pass_on(part, s):
            start(part, part, cs_sem.at[b, s], cr_sem.at[b, s], quad[1])

        mine = part_at(y, 0)
        start(mine, mine, gys_sem.at[b, 0], gyr_sem.at[b, 0], quad[2])
        gather_start(2, b, mine)
        pass_on(mine, 0)
        yield
        for k in (1, 3, 2):
            part = part_at(y, k)
            gather_wait(2, b, part, k)
            start(part, part, gys_sem.at[b, k], gyr_sem.at[b, k], quad[2])
            pass_on(part, k)
        yield
        for k in (0, 1, 3, 2):
            part = part_at(1 - y, k)
            remote(part, part, gys_sem.at[b, k], gyr_sem.at[b, k], quad[2]).wait_recv()
            pass_on(part, 4 + k)

    def cross(half_id, b):
        lanes = span(half_id * 256 + b * 128, 128)
        q_blk = q_rcv[b, half_id].astype(F32).T

        def score_step(i, carry):
            rows = span(i * 8, 8)
            scores[rows, :] = jnp.sum(ck[rows, :, lanes].astype(F32) * q_blk[None], axis=1)
            return carry

        lax.fori_loop(0, 8, score_step, 0)
        s = scores[...] + jnp.where(mask_ref[:, lanes] != 0, 0.0, NEG_FILL)
        e = jnp.exp(s - jnp.max(s, axis=0, keepdims=True))
        scores[...] = (e / jnp.sum(e, axis=0, keepdims=True)).astype(BF16).astype(F32)

        def mix_step(i, acc):
            p_blk = scores[span(i * 8, 8), :]
            for j in range(8):
                acc = acc + cv[i * 8 + j, :, lanes].astype(F32) * p_blk[j:j + 1, :]
            return acc

        return lax.fori_loop(0, 8, mix_step, jnp.zeros((64, 128), F32)).T.astype(BF16)

    def flow(b):
        for r in (1, 2, 3):
            att[b, r].wait_recv()
        heads[b] = jnp.concatenate([attn_ref[rows_of(b, 0), :]] + [att_rcv[b, r] for r in range(3)], axis=1)
        once("wo", local[2].wait, local[3].wait, to_core[0].wait_recv, to_core[1].wait_recv)
        total = yield from reduce_scatter(0, b, dot_nn(heads[b], wo4[...]))
        local[b].wait()
        resid = x_buf[b].astype(F32) + total
        h_buf[0, b, chunk(0, z)] = rms_norm(resid, nc_ref[...])
        yield from gather(0, b)
        once("cq", local[4].wait, local[5].wait, to_core[2].wait_recv, to_core[3].wait_recv)
        q4 = dot_nt(h_buf[0, b], cq4[...]).astype(BF16)
        for r in (3, 2, 1):
            q_snd[b, r - 1] = q4[:, r * 64:r * 64 + 64]
            start(q_snd.at[b, r - 1], q_rcv.at[b, c, span(y * 64, 64)], q_ssem.at[b, r - 1], q_rsem.at[b, r - 1], quad[r])
        q_rcv[b, c, span(y * 64, 64)] = q4[:, 0:64]
        yield
        once("kv", local[6].wait, local[7].wait)
        for half_id, pieces in ((c, (2,)), (1 - c, (1, 3))):
            for r in pieces:
                remote(q_snd.at[b, r - 1], q_rcv.at[b, quad_c[r], span(quad_y[r] * 64, 64)], q_ssem.at[b, r - 1], q_rsem.at[b, r - 1], quad[r]).wait_recv()
            o_buf[b, half_id] = cross(half_id, b)
            for r in reversed(pieces):
                start(o_buf.at[b, half_id, span(quad_y[r] * 64, 64)], o_rcv.at[b, r - 1], o_ssem.at[b, r - 1], o_rsem.at[b, r - 1], quad[r])
        if b == 1:
            start_wd()
        yield
        for r in (1, 2, 3):
            remote(o_buf.at[b, quad_c[r], span(quad_y[r] * 64, 64)], o_rcv.at[b, r - 1], o_ssem.at[b, r - 1], o_rsem.at[b, r - 1], quad[r]).wait_recv()
        heads[b] = jnp.concatenate([o_buf[b, c, span(y * 64, 64), :]] + [o_rcv[b, r] for r in range(3)], axis=1)
        once("co", local[8].wait, local[9].wait, to_core[4].wait_recv, to_core[5].wait_recv)
        partial = dot_nn(heads[b], co4[...])
        if b == 1:
            forward_gate_up()
        total = yield from reduce_scatter(1, b, partial)
        resid = resid + total
        h_buf[1, b, chunk(0, z)] = rms_norm(resid, nm_ref[...])
        yield from gather(1, b)
        if b == 0:
            forward_wd()
        once("gu", local[10].wait, local[11].wait, to_core[6].wait_recv, to_core[7].wait_recv, late["wg"].wait_recv, late["wu"].wait_recv)
        h = h_buf[1, b]
        act[b] = (gelu_tanh(dot_nt(h, wg4[...])) * dot_nt(h, wu4[...])).astype(BF16)
        once("wd", local[12].wait, to_core[8].wait_recv, late["wd3"].wait_recv)
        total = yield from reduce_scatter(2, b, dot_nn(act[b], wd4[...]))
        resid = resid + total
        out_ref[chunk(c * 256 + b * 128 + y * 64, z)] = resid.astype(BF16)
        yield from gather_out(b)

    flows = [flow(0), flow(1)]
    while flows:
        for item in list(flows):
            try:
                next(item)
            except StopIteration:
                flows.remove(item)
    for b in range(2):
        for s in range(8):
            yy = y if s < 4 else 1 - y
            part = out_ref.at[chunk((1 - c) * 256 + b * 128 + yy * 64, lax.rem(z + 4 - s % 4, 4))]
            remote(part, part, cs_sem.at[b, s], cr_sem.at[b, s], quad[1]).wait_recv()
    for copy in sends:
        copy.wait_send()


def tail(x_in, attn, mask_t, ck_t, cv_t, wo, cq_t, co, wg_t, wu_t, wd, woy, cqy_t, coy, nc, nm):
    hbm = pl.BlockSpec(memory_space=pltpu.HBM)
    anywhere = pl.BlockSpec(memory_space=pl.ANY)
    vmem = pl.BlockSpec(memory_space=pltpu.VMEM)
    units = wd.shape[0]
    dma = pltpu.SemaphoreType.DMA
    quarter = (256, 1024)
    scratch = [
        pltpu.VMEM((2, 16, 1024), BF16), pltpu.VMEM(ck_t.shape, BF16), pltpu.VMEM(cv_t.shape, BF16),
        pltpu.VMEM(quarter, BF16), pltpu.VMEM(quarter, BF16), pltpu.VMEM(quarter, BF16),
        pltpu.VMEM((4 * units, 1024), BF16), pltpu.VMEM((4 * units, 1024), BF16), pltpu.VMEM((4 * units, 1024), BF16),
        pltpu.VMEM((2, 3, 64, 64), BF16), pltpu.VMEM((2, 64, 256), BF16), pltpu.VMEM((2, 3, 64, 64), BF16), pltpu.VMEM((2, 2, 128, 64), BF16),
        pltpu.VMEM((2, 2, 128, 64), BF16), pltpu.VMEM((2, 3, 64, 64), BF16), pltpu.VMEM((64, 128), F32),
        pltpu.VMEM((2, 64, 1024), F32), pltpu.VMEM((3, 2, 64, 1024), BF16), pltpu.VMEM((3, 2, 3, 16, 1024), BF16), pltpu.VMEM((2, 2, 64, 1024), BF16),
        pltpu.VMEM((2, 64, 4 * units), BF16),
        dma((13,)), dma((15,)), dma((15,)), dma((2, 3)), dma((2, 3)), dma((2, 3)), dma((2, 3)), dma((2, 3)), dma((2, 3)),
        dma((3, 2, 3)), dma((3, 2, 3)), dma((3, 2, 3)), dma((3, 2, 3)), dma((2, 4)), dma((2, 4)), dma((2, 8)), dma((2, 8)),
    ]
    return pl.pallas_call(
        tail_kernel,
        out_shape=jax.ShapeDtypeStruct(x_in.shape, BF16),
        in_specs=[hbm, vmem, vmem] + [hbm] * 8 + [anywhere] * 3 + [vmem, vmem],
        out_specs=vmem,
        scratch_shapes=scratch,
        compiler_params=pltpu.CompilerParams(collective_id=0, has_side_effects=True, vmem_limit_bytes=60 * 1024 * 1024),
        name="tail",
    )(x_in, attn, mask_t, ck_t, cv_t, wo, cq_t, co, wg_t, wu_t, wd, woy, cqy_t, coy, nc, nm)


def head_kernel(tok_ref, rb_ref, x_ref, wq_ref, wk_ref, wv_ref, ns_ref, k_hbm, v_hbm,
                attn_ref, nk_hbm, nv_hbm,
                kbuf, vbuf, h_buf, qq, k_new, v_new, table, in_sem, out_sem):
    rows, depth, t_len = kbuf.shape
    n_chunks = in_sem.shape[1]
    size = rows // n_chunks

    def chunk_copy(i, which):
        hbm, buf = ((k_hbm, kbuf), (v_hbm, vbuf))[which]
        part = pl.ds(i * size, size)
        return pltpu.make_async_copy(hbm.at[part], buf.at[part], in_sem.at[which, i])

    def chunk_out(i, which):
        hbm, buf = ((nk_hbm, kbuf), (nv_hbm, vbuf))[which]
        part = pl.ds(i * size, size)
        return pltpu.make_async_copy(buf.at[part], hbm.at[part], out_sem.at[which, i])

    for i in range(n_chunks):
        chunk_copy(i, 0).start()
        chunk_copy(i, 1).start()

    distance = lax.broadcasted_iota(jnp.int32, (t_len, t_len), 0) - lax.broadcasted_iota(jnp.int32, (t_len, t_len), 1)
    bias = jnp.full((t_len, t_len), rb_ref[0], F32)
    for bucket, edge in enumerate(BUCKET_EDGES):
        bias = jnp.where(distance >= edge, rb_ref[bucket + 1], bias)
    table[...] = jnp.where(distance >= 0, bias, NEG_FILL)

    wqq = jnp.concatenate([wq_ref[...], wq_ref[...]], axis=0)
    for i in range(rows // 128):
        part = slice(i * 128, i * 128 + 128)
        h = rms_norm(x_ref[part, :].astype(F32), ns_ref[...])
        qq[part, :] = dot_nt(h, wqq).astype(BF16).astype(F32)
        k_new[i] = dot_nt(wk_ref[...], h).astype(BF16).astype(F32)
        v_new[i] = dot_nt(wv_ref[...], h).astype(BF16).astype(F32)

    lane = lax.broadcasted_iota(jnp.int32, (depth, t_len), 1)
    row8 = lax.broadcasted_iota(jnp.int32, (8, 128), 0)
    half8 = lax.broadcasted_iota(jnp.int32, (8, 128), 1) // depth

    def step(i, carry):
        chunk_copy(i, 0).wait()
        chunk_copy(i, 1).wait()
        shift = lax.rem(i, 2) * size
        k_cols = pltpu.roll(k_new[i // 2], shift, 1)
        v_cols = pltpu.roll(v_new[i // 2], shift, 1)
        scores = []
        for g in range(size // 8):
            k8, bias8 = [], []
            for j in range(8):
                b = i * size + g * 8 + j
                pos = tok_ref[b]
                at_pos = lane == pos
                col = g * 8 + j
                k_b = jnp.where(at_pos, jnp.broadcast_to(k_cols[:, col:col + 1], (depth, t_len)), kbuf[b].astype(F32)).astype(BF16)
                v_b = jnp.where(at_pos, jnp.broadcast_to(v_cols[:, col:col + 1], (depth, t_len)), vbuf[b].astype(F32)).astype(BF16)
                kbuf[b] = k_b
                vbuf[b] = v_b
                k8.append(k_b)
                bias8.append(table[pl.ds(pos, 1), :])
            q8 = qq[pl.ds(pl.multiple_of(i * size + g * 8, 8), 8), :]
            q_diag = jnp.concatenate([jnp.where(row8 == 2 * m + half8, q8, 0.0) for m in range(4)], axis=1).astype(BF16)
            scores.append(dot_nn(q_diag, jnp.concatenate(k8, axis=0)) + jnp.concatenate(bias8, axis=0))
        chunk_out(i, 0).start()
        chunk_out(i, 1).start()
        s = jnp.concatenate(scores, axis=0)
        e = jnp.exp(s - jnp.max(s, axis=1, keepdims=True))
        p = (e / jnp.sum(e, axis=1, keepdims=True)).astype(BF16).astype(F32)
        outs = []
        for g in range(size // 8):
            p8 = p[g * 8:g * 8 + 8, :]
            p_diag = jnp.concatenate([jnp.where(row8 == j, p8, 0.0) for j in range(8)], axis=1).astype(BF16)
            v8 = jnp.concatenate([vbuf[i * size + g * 8 + j] for j in range(8)], axis=1)
            outs.append(dot_nt(p_diag, v8))
        attn_ref[pl.ds(pl.multiple_of(i * size, size), size), :] = jnp.concatenate(outs, axis=0).astype(BF16)
        return carry

    lax.fori_loop(0, n_chunks, step, 0)
    for i in range(n_chunks):
        chunk_out(i, 0).wait()
        chunk_out(i, 1).wait()


def head(tok_pos, rel_bias, x_in, wq_t, wk_t, wv_t, ns, k_t, v_t):
    hbm = pl.BlockSpec(memory_space=pltpu.HBM)
    vmem = pl.BlockSpec(memory_space=pltpu.VMEM)
    smem = pl.BlockSpec(memory_space=pltpu.SMEM)
    rows, depth, t_len = k_t.shape
    dma = pltpu.SemaphoreType.DMA
    n_chunks = 8
    return pl.pallas_call(
        head_kernel,
        out_shape=(jax.ShapeDtypeStruct((rows, depth), BF16), jax.ShapeDtypeStruct(k_t.shape, BF16), jax.ShapeDtypeStruct(v_t.shape, BF16)),
        in_specs=[smem, smem] + [vmem] * 5 + [hbm] * 2,
        out_specs=(vmem, hbm, hbm),
        scratch_shapes=[
            pltpu.VMEM(k_t.shape, BF16), pltpu.VMEM(v_t.shape, BF16), pltpu.VMEM((8, 128), BF16),
            pltpu.VMEM((rows, 2 * depth), F32), pltpu.VMEM((rows // 128, depth, 128), F32), pltpu.VMEM((rows // 128, depth, 128), F32),
            pltpu.VMEM((t_len, t_len), F32), dma((2, n_chunks)), dma((2, n_chunks)),
        ],
        compiler_params=pltpu.CompilerParams(vmem_limit_bytes=60 * 1024 * 1024),
        cost_estimate=pl.CostEstimate(flops=4 * 10**9, bytes_accessed=34 * 1024 * 1024, transcendentals=65536),
        name="head",
    )(tok_pos, rel_bias, x_in, wq_t, wk_t, wv_t, ns, k_t, v_t)


def solution(mesh):
    def local_layer(x_in, tok_pos, self_k, self_v, cross_k, cross_v, enc_mask, rel_bias, w_q, w_k, w_v, w_o, cross_q, cross_o, w_gate, w_up, w_down, norm_self, norm_cross, norm_mlp):
        k_t = jnp.transpose(self_k[:, :, 0, :], (0, 2, 1))
        v_t = jnp.transpose(self_v[:, :, 0, :], (0, 2, 1))
        attn, new_k, new_v = head(tok_pos, rel_bias[:, 0], x_in, w_q.T, w_k.T, w_v.T, norm_self, k_t, v_t)
        new_self_k = jnp.transpose(new_k, (0, 2, 1))[:, :, None, :]
        new_self_v = jnp.transpose(new_v, (0, 2, 1))[:, :, None, :]
        ck_t = jnp.transpose(cross_k[:, :, 0, :], (1, 2, 0))
        cv_t = jnp.transpose(cross_v[:, :, 0, :], (1, 2, 0))
        tp_size = mesh.shape["tp"]
        across_y = [(i, i ^ 2) for i in range(tp_size)]
        wo_y, cq_y, co_y = (lax.ppermute(w, "tp", across_y) for w in (w_o, cross_q.T, cross_o))
        out = tail(x_in, attn, enc_mask.T, ck_t, cv_t, w_o, cross_q.T, cross_o, w_gate.T, w_up.T, w_down, wo_y, cq_y, co_y,
                   norm_cross, norm_mlp)
        return out, new_self_k, new_self_v

    cache_spec = P('dp', None, 'tp', None)
    split_cols = P(None, 'tp')
    split_rows = P('tp', None)
    in_specs = (P('dp', None), P('dp'), cache_spec, cache_spec, cache_spec, cache_spec, P('dp', None), split_cols, split_cols, split_cols, split_cols, split_rows, split_cols, split_rows, split_cols, split_cols, split_rows, P(None), P(None), P(None))
    out_specs = (P('dp', None), cache_spec, cache_spec)
    return jax.shard_map(local_layer, mesh=mesh, in_specs=in_specs, out_specs=out_specs, check_vma=False)
```

```python
import math
import jax
import jax.numpy as jnp
from jax import lax
from jax.experimental import pallas as pl
from jax.experimental.pallas import tpu as pltpu
from jax.sharding import PartitionSpec as P

BUCKET_EDGES = tuple(range(1, 16)) + (16,) + tuple(int(math.ceil(16.0 * 8.0 ** (m / 16.0))) for m in range(1, 16))
NEG_FILL = -1e30
MESH = pl.DeviceIdType.MESH
F32 = jnp.float32
BF16 = jnp.bfloat16
K_ORDER = (2, 1, 3)
Y_FIRST, Y_SECOND, Y_THIRD = ("cq", "co", "wg"), ("wu",), ("wv", "wd")
VMEM_BYTES = 60 * 1024 * 1024


def rms_norm(values, norm_scale):
    inv_rms = lax.rsqrt(jnp.mean(values * values, axis=-1, keepdims=True) + 1e-6)
    return (values * inv_rms * norm_scale.astype(F32)[None, :]).astype(BF16)


def gelu_tanh(u):
    return u * (0.5 * (1.0 + jnp.tanh(math.sqrt(2.0 / math.pi) * (u + 0.044715 * (u * u * u)))))


def dot_nt(a, b):
    return lax.dot_general(a, b, (((1,), (1,)), ((), ())), preferred_element_type=F32)


def dot_nn(a, b):
    return jnp.dot(a, b, preferred_element_type=F32)


def tail_kernel(x_hbm, attn_ref, mask_ref, ck_hbm, cv_hbm, wo_ref, cq_hbm, co_hbm, wg_hbm, wu_hbm, wd_hbm, woy_hbm, nc_ref, nm_ref,
                out_ref,
                x_buf, ck, cv, wo4, cq4, co4, wg4, wu4, wd4, att_rcv, heads, q_snd, q_rcv, o_buf, o_rcv, scores,
                own, z_snd, z_rcv, h_buf, act,
                loc_sem, wo_ssem, wo_rsem, w_ssem, w_rsem, at_ssem, at_rsem, q_ssem, q_rsem, o_ssem, o_rsem, zs_sem, zr_sem, gzs_sem, gzr_sem, gys_sem, gyr_sem, cs_sem, cr_sem):
    me = lax.axis_index("tp")
    c = lax.rem(me, 2)
    y = lax.rem(me // 2, 2)
    z = me // 4
    quad = {r: {"tp": z * 4 + (y if r < 2 else 1 - y) * 2 + (c if r == 2 else 1 - c)} for r in (1, 2, 3)}
    quad_c = {0: c, 1: 1 - c, 2: c, 3: 1 - c}
    quad_y = {0: y, 1: y, 2: 1 - y, 3: 1 - y}
    z_peer = {k: {"tp": lax.rem(z + k, 4) * 4 + y * 2 + c} for k in (1, 2, 3)}
    sends = []

    def remote(src, dst, ssem, rsem, peer):
        return pltpu.make_async_remote_copy(src_ref=src, dst_ref=dst, send_sem=ssem, recv_sem=rsem, device_id=peer, device_id_type=MESH)

    def start(src, dst, ssem, rsem, peer):
        copy = remote(src, dst, ssem, rsem, peer)
        copy.start()
        sends.append(copy)
        return copy

    def span(base, size):
        return pl.ds(pl.multiple_of(base, size), size)

    def chunk(base, zz):
        return span(base + zz * 16, 16)

    def slot(ref, r):
        size = ref.shape[0] // 4
        return ref.at[pl.ds(r * size, size)]

    local = [pltpu.make_async_copy(src, dst, loc_sem.at[i]) for i, (src, dst) in enumerate((
        (x_hbm.at[chunk(c * 256 + y * 64, z)], x_buf.at[0]),
        (x_hbm.at[chunk(c * 256 + 128 + y * 64, z)], x_buf.at[1]),
        (wo_ref, slot(wo4, 0)), (woy_hbm, slot(wo4, 2)), (cq_hbm, slot(cq4, 0)), (ck_hbm, ck), (cv_hbm, cv), (co_hbm, slot(co4, 0)),
        (wg_hbm, slot(wg4, 0)), (wu_hbm, slot(wu4, 0)), (wd_hbm, slot(wd4, 0)),
    ))]
    for copy in local:
        copy.start()

    barrier = pltpu.get_barrier_semaphore()
    for peer in (quad[1], quad[2], quad[3], z_peer[1], z_peer[2], z_peer[3]):
        pl.semaphore_signal(barrier, inc=1, device_id=peer, device_id_type=MESH)
    pl.semaphore_wait(barrier, 6)

    def rows_of(b, r):
        return span(quad_c[r] * 256 + b * 128 + quad_y[r] * 64, 64)

    att = {}
    for b in range(2):
        for r in (3, 2, 1):
            att[b, r] = start(attn_ref.at[rows_of(b, r)], att_rcv.at[b, r - 1], at_ssem.at[b, r - 1], at_rsem.at[b, r - 1], quad[r])
    part = 96
    pieces = {
        "cq": (cq_hbm, cq4, 0, cq_hbm.shape[0]), "co": (co_hbm, co4, 0, co_hbm.shape[0]),
        "wg": (wg_hbm, wg4, 0, wg_hbm.shape[0]), "wu": (wu_hbm, wu4, 0, part), "wv": (wu_hbm, wu4, part, wu_hbm.shape[0] - part),
        "wd": (wd_hbm, wd4, 0, wd_hbm.shape[0]),
    }
    w_copy = {}

    def send_weight(name, r):
        src, slots, first, size = pieces[name]
        rows = pl.ds(first, size)
        if r == 3:
            w_copy[name, 2].wait_recv()
            src = slot(slots, 2)
        i = list(pieces).index(name)
        w_copy[name, r] = start(src.at[rows], slot(slots, r).at[rows], w_ssem.at[i, r - 1], w_rsem.at[i, r - 1], quad[2 if r == 2 else 1])

    def weight_waits(*names):
        return [w_copy[name, r].wait_recv for name in names for r in (1, 3)]

    wo_copies = [start(src, slot(wo4, r), wo_ssem.at[r // 2], wo_rsem.at[r // 2], quad[1]) for src, r in ((wo_ref, 1), (woy_hbm, 3))]
    for name in pieces:
        send_weight(name, 1)
    for name in Y_FIRST:
        send_weight(name, 2)

    def once(*waits):
        for wait in waits:
            wait()

    def reduce_scatter(p, b, partial, then=None):
        own[b] = partial
        z_snd[p, b] = partial.astype(BF16)
        copies = {}
        for k in K_ORDER:
            copies[k] = start(z_snd.at[p, b, chunk(0, lax.rem(z + k, 4))], z_rcv.at[p, b, k - 1], zs_sem.at[p, b, k - 1], zr_sem.at[p, b, k - 1], z_peer[k])
        if then is not None:
            then()
        yield
        total = own[b, chunk(0, z)]
        for k in (1, 3, 2):
            copies[k].wait_recv()
            total = total + z_rcv[p, b, k - 1].astype(F32)
        return total

    def gather_start(p, b, mine):
        for k in K_ORDER:
            start(mine, mine, gzs_sem.at[p, b, k - 1], gzr_sem.at[p, b, k - 1], z_peer[k])

    def gather_wait(p, b, part, k):
        remote(part, part, gzs_sem.at[p, b, k - 1], gzr_sem.at[p, b, k - 1], z_peer[k]).wait_recv()

    def gather(p, b, then=None):
        buf = h_buf.at[p, b]
        gather_start(p, b, buf.at[chunk(0, z)])
        if then is not None:
            then()
        yield
        for k in (1, 3, 2):
            gather_wait(p, b, buf.at[chunk(0, lax.rem(z + 4 - k, 4))], k)

    def gather_out(b):
        first = c * 256 + b * 128

        def part_at(yy, k):
            return out_ref.at[chunk(first + yy * 64, lax.rem(z + 4 - k, 4))]

        def pass_on(part, s):
            start(part, part, cs_sem.at[b, s], cr_sem.at[b, s], quad[1])

        mine = part_at(y, 0)
        start(mine, mine, gys_sem.at[b, 0], gyr_sem.at[b, 0], quad[2])
        gather_start(2, b, mine)
        pass_on(mine, 0)
        yield
        for k in (1, 3, 2):
            part = part_at(y, k)
            gather_wait(2, b, part, k)
            start(part, part, gys_sem.at[b, k], gyr_sem.at[b, k], quad[2])
            pass_on(part, k)
        yield
        for k in (0, 1, 3, 2):
            part = part_at(1 - y, k)
            remote(part, part, gys_sem.at[b, k], gyr_sem.at[b, k], quad[2]).wait_recv()
            pass_on(part, 4 + k)

    def cross(half_id, b):
        lanes = span(half_id * 256 + b * 128, 128)
        q_blk = q_rcv[b, half_id].astype(F32).T

        def score_step(i, carry):
            rows = span(i * 8, 8)
            scores[rows, :] = jnp.sum(ck[rows, :, lanes].astype(F32) * q_blk[None], axis=1)
            return carry

        lax.fori_loop(0, 8, score_step, 0)
        s = scores[...] + jnp.where(mask_ref[:, lanes] != 0, 0.0, NEG_FILL)
        e = jnp.exp(s - jnp.max(s, axis=0, keepdims=True))
        scores[...] = (e / jnp.sum(e, axis=0, keepdims=True)).astype(BF16).astype(F32)

        def mix_step(i, acc):
            p_blk = scores[span(i * 8, 8), :]
            for j in range(8):
                acc = acc + cv[i * 8 + j, :, lanes].astype(F32) * p_blk[j:j + 1, :]
            return acc

        return lax.fori_loop(0, 8, mix_step, jnp.zeros((64, 128), F32)).T.astype(BF16)

    def flow(b):
        for r in (1, 2, 3):
            att[b, r].wait_recv()
        heads[b] = jnp.concatenate([attn_ref[rows_of(b, 0), :]] + [att_rcv[b, r] for r in range(3)], axis=1)
        if b == 0:
            once(local[2].wait, local[3].wait, *[copy.wait_recv for copy in wo_copies])
        partial = dot_nn(heads[b], wo4[...])
        total = yield from reduce_scatter(0, b, partial, (lambda: send_weight("cq", 3)) if b == 1 else None)
        local[b].wait()
        resid = x_buf[b].astype(F32) + total
        h_buf[0, b, chunk(0, z)] = rms_norm(resid, nc_ref[...])
        yield from gather(0, b)
        if b == 0:
            once(local[4].wait, *weight_waits("cq"))
        q4 = dot_nt(h_buf[0, b], cq4[...]).astype(BF16)
        for r in (3, 2, 1):
            q_snd[b, r - 1] = q4[:, r * 64:r * 64 + 64]
            start(q_snd.at[b, r - 1], q_rcv.at[b, c, span(y * 64, 64)], q_ssem.at[b, r - 1], q_rsem.at[b, r - 1], quad[r])
        q_rcv[b, c, span(y * 64, 64)] = q4[:, 0:64]
        if b == 0:
            send_weight("co", 3)
        else:
            for name in Y_SECOND:
                send_weight(name, 2)
        yield
        if b == 0:
            once(local[5].wait, local[6].wait)
        for half_id, pieces in ((c, (2,)), (1 - c, (1, 3))):
            for r in pieces:
                remote(q_snd.at[b, r - 1], q_rcv.at[b, quad_c[r], span(quad_y[r] * 64, 64)], q_ssem.at[b, r - 1], q_rsem.at[b, r - 1], quad[r]).wait_recv()
            o_buf[b, half_id] = cross(half_id, b)
            for r in reversed(pieces):
                start(o_buf.at[b, half_id, span(quad_y[r] * 64, 64)], o_rcv.at[b, r - 1], o_ssem.at[b, r - 1], o_rsem.at[b, r - 1], quad[r])
        if b == 1:
            for name in Y_THIRD:
                send_weight(name, 2)
            send_weight("wg", 3)
        yield
        for r in (1, 2, 3):
            remote(o_buf.at[b, quad_c[r], span(quad_y[r] * 64, 64)], o_rcv.at[b, r - 1], o_ssem.at[b, r - 1], o_rsem.at[b, r - 1], quad[r]).wait_recv()
        heads[b] = jnp.concatenate([o_buf[b, c, span(y * 64, 64), :]] + [o_rcv[b, r] for r in range(3)], axis=1)
        if b == 0:
            once(local[7].wait, *weight_waits("co"))
        partial = dot_nn(heads[b], co4[...])
        total = yield from reduce_scatter(1, b, partial, (lambda: send_weight("wu", 3)) if b == 1 else None)
        resid = resid + total
        h_buf[1, b, chunk(0, z)] = rms_norm(resid, nm_ref[...])
        yield from gather(1, b, (lambda: send_weight("wv", 3)) if b == 1 else None)
        if b == 0:
            send_weight("wd", 3)
            once(*[copy.wait for copy in local[8:]], *weight_waits("wg", "wu", "wv"))
        h = h_buf[1, b]
        act[b] = (gelu_tanh(dot_nt(h, wg4[...])) * dot_nt(h, wu4[...])).astype(BF16)
        if b == 0:
            once(*weight_waits("wd"))
        total = yield from reduce_scatter(2, b, dot_nn(act[b], wd4[...]))
        resid = resid + total
        out_ref[chunk(c * 256 + b * 128 + y * 64, z)] = resid.astype(BF16)
        yield from gather_out(b)

    flows = [flow(0), flow(1)]
    while flows:
        for item in list(flows):
            try:
                next(item)
            except StopIteration:
                flows.remove(item)
    for b in range(2):
        for s in range(8):
            yy = y if s < 4 else 1 - y
            part = out_ref.at[chunk((1 - c) * 256 + b * 128 + yy * 64, lax.rem(z + 4 - s % 4, 4))]
            remote(part, part, cs_sem.at[b, s], cr_sem.at[b, s], quad[1]).wait_recv()
    for copy in sends:
        copy.wait_send()


def tail(x_in, attn, mask_t, ck_t, cv_t, wo, cq_t, co, wg_t, wu_t, wd, woy, nc, nm):
    hbm = pl.BlockSpec(memory_space=pltpu.HBM)
    vmem = pl.BlockSpec(memory_space=pltpu.VMEM)
    units, wide = wd.shape
    deep = wo.shape[0]
    dma = pltpu.SemaphoreType.DMA
    bf16_shapes = [(2, 16, wide), ck_t.shape, cv_t.shape] + [(4 * deep, wide)] * 3 + [(4 * units, wide)] * 3
    bf16_shapes += [(2, 3, 64, deep), (2, 64, 4 * deep), (2, 3, 64, deep), (2, 2, 128, deep), (2, 2, 128, deep), (2, 3, 64, deep)]
    z_shapes = [(3, 2, 64, wide), (3, 2, 3, 16, wide), (2, 2, 64, wide), (2, 64, 4 * units)]
    sems = [(11,), (2,), (2,), (6, 3), (6, 3)] + [(2, 3)] * 6 + [(3, 2, 3)] * 4 + [(2, 4)] * 2 + [(2, 8)] * 2
    scratch = [pltpu.VMEM(shape, BF16) for shape in bf16_shapes]
    scratch += [pltpu.VMEM((deep, 128), F32), pltpu.VMEM((2, 64, wide), F32)]
    scratch += [pltpu.VMEM(shape, BF16) for shape in z_shapes] + [dma(shape) for shape in sems]
    return pl.pallas_call(
        tail_kernel,
        out_shape=jax.ShapeDtypeStruct(x_in.shape, BF16),
        in_specs=[hbm, vmem, vmem, hbm, hbm, vmem] + [hbm] * 6 + [vmem, vmem],
        out_specs=vmem,
        scratch_shapes=scratch,
        compiler_params=pltpu.CompilerParams(collective_id=0, has_side_effects=True, vmem_limit_bytes=VMEM_BYTES),
        name="tail",
    )(x_in, attn, mask_t, ck_t, cv_t, wo, cq_t, co, wg_t, wu_t, wd, woy, nc, nm)


def head_kernel(tok_ref, rb_ref, x_ref, wq_ref, wk_ref, wv_ref, ns_ref, k_hbm, v_hbm,
                attn_ref, nk_hbm, nv_hbm,
                kbuf, vbuf, h_buf, qq, k_new, v_new, table, in_sem, out_sem):
    rows, depth, t_len = kbuf.shape
    n_chunks = in_sem.shape[1]
    size = rows // n_chunks

    def chunk_copy(i, which):
        hbm, buf = ((k_hbm, kbuf), (v_hbm, vbuf))[which]
        part = pl.ds(i * size, size)
        return pltpu.make_async_copy(hbm.at[part], buf.at[part], in_sem.at[which, i])

    def chunk_out(i, which):
        hbm, buf = ((nk_hbm, kbuf), (nv_hbm, vbuf))[which]
        part = pl.ds(i * size, size)
        return pltpu.make_async_copy(buf.at[part], hbm.at[part], out_sem.at[which, i])

    for i in range(n_chunks):
        chunk_copy(i, 0).start()
        chunk_copy(i, 1).start()

    distance = lax.broadcasted_iota(jnp.int32, (t_len, t_len), 0) - lax.broadcasted_iota(jnp.int32, (t_len, t_len), 1)
    bias = jnp.full((t_len, t_len), rb_ref[0], F32)
    for bucket, edge in enumerate(BUCKET_EDGES):
        bias = jnp.where(distance >= edge, rb_ref[bucket + 1], bias)
    table[...] = jnp.where(distance >= 0, bias, NEG_FILL)

    wqq = jnp.concatenate([wq_ref[...], wq_ref[...]], axis=0)
    for i in range(rows // 128):
        part = slice(i * 128, i * 128 + 128)
        h = rms_norm(x_ref[part, :].astype(F32), ns_ref[...])
        qq[part, :] = dot_nt(h, wqq).astype(BF16).astype(F32)
        k_new[i] = dot_nt(wk_ref[...], h).astype(BF16).astype(F32)
        v_new[i] = dot_nt(wv_ref[...], h).astype(BF16).astype(F32)

    lane = lax.broadcasted_iota(jnp.int32, (depth, t_len), 1)
    row8 = lax.broadcasted_iota(jnp.int32, (8, 128), 0)
    half8 = lax.broadcasted_iota(jnp.int32, (8, 128), 1) // depth

    def step(i, carry):
        chunk_copy(i, 0).wait()
        chunk_copy(i, 1).wait()
        shift = lax.rem(i, 2) * size
        k_cols = pltpu.roll(k_new[i // 2], shift, 1)
        v_cols = pltpu.roll(v_new[i // 2], shift, 1)
        scores = []
        for g in range(size // 8):
            k8, bias8 = [], []
            for j in range(8):
                b = i * size + g * 8 + j
                pos = tok_ref[b]
                at_pos = lane == pos
                col = g * 8 + j
                k_b = jnp.where(at_pos, jnp.broadcast_to(k_cols[:, col:col + 1], (depth, t_len)), kbuf[b].astype(F32)).astype(BF16)
                v_b = jnp.where(at_pos, jnp.broadcast_to(v_cols[:, col:col + 1], (depth, t_len)), vbuf[b].astype(F32)).astype(BF16)
                kbuf[b] = k_b
                vbuf[b] = v_b
                k8.append(k_b)
                bias8.append(table[pl.ds(pos, 1), :])
            q8 = qq[pl.ds(pl.multiple_of(i * size + g * 8, 8), 8), :]
            q_diag = jnp.concatenate([jnp.where(row8 == 2 * m + half8, q8, 0.0) for m in range(4)], axis=1).astype(BF16)
            scores.append(dot_nn(q_diag, jnp.concatenate(k8, axis=0)) + jnp.concatenate(bias8, axis=0))
        chunk_out(i, 0).start()
        chunk_out(i, 1).start()
        s = jnp.concatenate(scores, axis=0)
        e = jnp.exp(s - jnp.max(s, axis=1, keepdims=True))
        p = (e / jnp.sum(e, axis=1, keepdims=True)).astype(BF16).astype(F32)
        outs = []
        for g in range(size // 8):
            p8 = p[g * 8:g * 8 + 8, :]
            p_diag = jnp.concatenate([jnp.where(row8 == j, p8, 0.0) for j in range(8)], axis=1).astype(BF16)
            v8 = jnp.concatenate([vbuf[i * size + g * 8 + j] for j in range(8)], axis=1)
            outs.append(dot_nt(p_diag, v8))
        attn_ref[pl.ds(pl.multiple_of(i * size, size), size), :] = jnp.concatenate(outs, axis=0).astype(BF16)
        return carry

    lax.fori_loop(0, n_chunks, step, 0)
    for i in range(n_chunks):
        chunk_out(i, 0).wait()
        chunk_out(i, 1).wait()


def head(tok_pos, rel_bias, x_in, wq_t, wk_t, wv_t, ns, k_t, v_t):
    hbm = pl.BlockSpec(memory_space=pltpu.HBM)
    vmem = pl.BlockSpec(memory_space=pltpu.VMEM)
    smem = pl.BlockSpec(memory_space=pltpu.SMEM)
    rows, depth, t_len = k_t.shape
    dma = pltpu.SemaphoreType.DMA
    n_chunks = 8
    return pl.pallas_call(
        head_kernel,
        out_shape=(jax.ShapeDtypeStruct((rows, depth), BF16), jax.ShapeDtypeStruct(k_t.shape, BF16), jax.ShapeDtypeStruct(v_t.shape, BF16)),
        in_specs=[smem, smem] + [vmem] * 5 + [hbm] * 2,
        out_specs=(vmem, hbm, hbm),
        scratch_shapes=[
            pltpu.VMEM(k_t.shape, BF16), pltpu.VMEM(v_t.shape, BF16), pltpu.VMEM((8, 128), BF16),
            pltpu.VMEM((rows, 2 * depth), F32), pltpu.VMEM((rows // 128, depth, 128), F32), pltpu.VMEM((rows // 128, depth, 128), F32),
            pltpu.VMEM((t_len, t_len), F32), dma((2, n_chunks)), dma((2, n_chunks)),
        ],
        compiler_params=pltpu.CompilerParams(vmem_limit_bytes=VMEM_BYTES),
        cost_estimate=pl.CostEstimate(flops=4 * 10**9, bytes_accessed=34 * 2**20, transcendentals=2**16),
        name="head",
    )(tok_pos, rel_bias, x_in, wq_t, wk_t, wv_t, ns, k_t, v_t)


def solution(mesh):
    def local_layer(x_in, tok_pos, self_k, self_v, cross_k, cross_v, enc_mask, rel_bias, w_q, w_k, w_v, w_o, cross_q, cross_o, w_gate, w_up, w_down, norm_self, norm_cross, norm_mlp):
        k_t = jnp.transpose(self_k[:, :, 0, :], (0, 2, 1))
        v_t = jnp.transpose(self_v[:, :, 0, :], (0, 2, 1))
        attn, new_k, new_v = head(tok_pos, rel_bias[:, 0], x_in, w_q.T, w_k.T, w_v.T, norm_self, k_t, v_t)
        new_self_k = jnp.transpose(new_k, (0, 2, 1))[:, :, None, :]
        new_self_v = jnp.transpose(new_v, (0, 2, 1))[:, :, None, :]
        ck_t = jnp.transpose(cross_k[:, :, 0, :], (1, 2, 0))
        cv_t = jnp.transpose(cross_v[:, :, 0, :], (1, 2, 0))
        wo_y = lax.ppermute(w_o, "tp", [(i, i ^ 2) for i in range(mesh.shape["tp"])])
        out = tail(x_in, attn, enc_mask.T, ck_t, cv_t, w_o, cross_q.T, cross_o, w_gate.T, w_up.T, w_down, wo_y, norm_cross, norm_mlp)
        return out, new_self_k, new_self_v

    cache_spec = P('dp', None, 'tp', None)
    split_cols = P(None, 'tp')
    split_rows = P('tp', None)
    in_specs = (P('dp', None), P('dp'), cache_spec, cache_spec, cache_spec, cache_spec, P('dp', None), split_cols, split_cols, split_cols, split_cols, split_rows, split_cols, split_rows, split_cols, split_cols, split_rows, P(None), P(None), P(None))
    out_specs = (P('dp', None), cache_spec, cache_spec)
    return jax.shard_map(local_layer, mesh=mesh, in_specs=in_specs, out_specs=out_specs, check_vma=False)
```

```python
import math
import jax
import jax.numpy as jnp
from jax import lax
from jax.experimental import pallas as pl
from jax.experimental.pallas import tpu as pltpu
from jax.sharding import PartitionSpec as P

BUCKET_EDGES = tuple(range(1, 16)) + (16,) + tuple(int(math.ceil(16.0 * 8.0 ** (m / 16.0))) for m in range(1, 16))
NEG_FILL = -1e30
MESH = pl.DeviceIdType.MESH
F32 = jnp.float32
BF16 = jnp.bfloat16
K_ORDER = (2, 1, 3)
Y_FIRST, Y_SECOND, Y_THIRD = ("cq", "co", "wg"), ("wu",), ("wv", "wd")
VMEM_BYTES = 60 * 1024 * 1024


def rms_norm(values, norm_scale):
    inv_rms = lax.rsqrt(jnp.mean(values * values, axis=-1, keepdims=True) + 1e-6)
    return (values * inv_rms * norm_scale.astype(F32)[None, :]).astype(BF16)


def gelu_tanh(u):
    return u * (0.5 * (1.0 + jnp.tanh(math.sqrt(2.0 / math.pi) * (u + 0.044715 * (u * u * u)))))


def dot_nt(a, b):
    return lax.dot_general(a, b, (((1,), (1,)), ((), ())), preferred_element_type=F32)


def dot_nn(a, b):
    return jnp.dot(a, b, preferred_element_type=F32)


def tail_kernel(x_hbm, attn_ref, mask_ref, ck_hbm, cv_hbm, wo_ref, cq_hbm, co_hbm, wg_hbm, wu_hbm, wd_hbm, woy_hbm, nc_ref, nm_ref,
                out_ref,
                x_buf, ck, cv, wo4, cq4, co4, wg4, wu4, wd4, att_rcv, heads, q_snd, q_rcv, o_buf, o_rcv, scores,
                own, z_snd, z_rcv, h_buf, act,
                loc_sem, wo_ssem, wo_rsem, w_ssem, w_rsem, at_ssem, at_rsem, q_ssem, q_rsem, o_ssem, o_rsem, zs_sem, zr_sem, gzs_sem, gzr_sem, gys_sem, gyr_sem, cs_sem, cr_sem):
    me = lax.axis_index("tp")
    c = lax.rem(me, 2)
    y = lax.rem(me // 2, 2)
    z = me // 4
    quad = {r: {"tp": z * 4 + (y if r < 2 else 1 - y) * 2 + (c if r == 2 else 1 - c)} for r in (1, 2, 3)}
    quad_c = {0: c, 1: 1 - c, 2: c, 3: 1 - c}
    quad_y = {0: y, 1: y, 2: 1 - y, 3: 1 - y}
    z_peer = {k: {"tp": lax.rem(z + k, 4) * 4 + y * 2 + c} for k in (1, 2, 3)}
    sends = []

    def remote(src, dst, ssem, rsem, peer):
        return pltpu.make_async_remote_copy(src_ref=src, dst_ref=dst, send_sem=ssem, recv_sem=rsem, device_id=peer, device_id_type=MESH)

    def start(src, dst, ssem, rsem, peer):
        copy = remote(src, dst, ssem, rsem, peer)
        copy.start()
        sends.append(copy)
        return copy

    def span(base, size):
        return pl.ds(pl.multiple_of(base, size), size)

    def chunk(base, zz):
        return span(base + zz * 16, 16)

    def slot(ref, r):
        size = ref.shape[0] // 4
        return ref.at[pl.ds(r * size, size)]

    local = [pltpu.make_async_copy(src, dst, loc_sem.at[i]) for i, (src, dst) in enumerate((
        (x_hbm.at[chunk(c * 256 + y * 64, z)], x_buf.at[0]),
        (x_hbm.at[chunk(c * 256 + 128 + y * 64, z)], x_buf.at[1]),
        (wo_ref, slot(wo4, 0)), (woy_hbm, slot(wo4, 2)), (cq_hbm, slot(cq4, 0)), (ck_hbm, ck), (cv_hbm, cv), (co_hbm, slot(co4, 0)),
        (wg_hbm, slot(wg4, 0)), (wu_hbm, slot(wu4, 0)), (wd_hbm, slot(wd4, 0)),
    ))]
    for copy in local:
        copy.start()

    barrier = pltpu.get_barrier_semaphore()
    for peer in (quad[1], quad[2], quad[3], z_peer[1], z_peer[2], z_peer[3]):
        pl.semaphore_signal(barrier, inc=1, device_id=peer, device_id_type=MESH)
    pl.semaphore_wait(barrier, 6)

    def rows_of(b, r):
        return span(quad_c[r] * 256 + b * 128 + quad_y[r] * 64, 64)

    att = {}
    for b in range(2):
        for r in (3, 2, 1):
            att[b, r] = start(attn_ref.at[rows_of(b, r)], att_rcv.at[b, r - 1], at_ssem.at[b, r - 1], at_rsem.at[b, r - 1], quad[r])
    part = 96
    pieces = {
        "cq": (cq_hbm, cq4, 0, cq_hbm.shape[0]), "co": (co_hbm, co4, 0, co_hbm.shape[0]),
        "wg": (wg_hbm, wg4, 0, wg_hbm.shape[0]), "wu": (wu_hbm, wu4, 0, part), "wv": (wu_hbm, wu4, part, wu_hbm.shape[0] - part),
        "wd": (wd_hbm, wd4, 0, wd_hbm.shape[0]),
    }
    w_copy = {}

    def send_weight(name, r):
        src, slots, first, size = pieces[name]
        rows = pl.ds(first, size)
        if r == 3:
            w_copy[name, 2].wait_recv()
            src = slot(slots, 2)
        i = list(pieces).index(name)
        w_copy[name, r] = start(src.at[rows], slot(slots, r).at[rows], w_ssem.at[i, r - 1], w_rsem.at[i, r - 1], quad[2 if r == 2 else 1])

    def weight_waits(*names):
        return [w_copy[name, r].wait_recv for name in names for r in (1, 3)]

    wo_copies = [start(src, slot(wo4, r), wo_ssem.at[r // 2], wo_rsem.at[r // 2], quad[1]) for src, r in ((wo_ref, 1), (woy_hbm, 3))]
    for name in pieces:
        send_weight(name, 1)
    for name in Y_FIRST:
        send_weight(name, 2)

    def once(*waits):
        for wait in waits:
            wait()

    def reduce_scatter(p, b, partial, then=None):
        own[b] = partial
        z_snd[p, b] = partial.astype(BF16)
        copies = {}
        for k in K_ORDER:
            copies[k] = start(z_snd.at[p, b, chunk(0, lax.rem(z + k, 4))], z_rcv.at[p, b, k - 1], zs_sem.at[p, b, k - 1], zr_sem.at[p, b, k - 1], z_peer[k])
        if then is not None:
            then()
        yield
        total = own[b, chunk(0, z)]
        for k in (1, 3, 2):
            copies[k].wait_recv()
            total = total + z_rcv[p, b, k - 1].astype(F32)
        return total

    def gather_start(p, b, mine):
        for k in K_ORDER:
            start(mine, mine, gzs_sem.at[p, b, k - 1], gzr_sem.at[p, b, k - 1], z_peer[k])

    def gather_wait(p, b, part, k):
        remote(part, part, gzs_sem.at[p, b, k - 1], gzr_sem.at[p, b, k - 1], z_peer[k]).wait_recv()

    def gather(p, b, then=None):
        buf = h_buf.at[p, b]
        gather_start(p, b, buf.at[chunk(0, z)])
        if then is not None:
            then()
        yield
        for k in (1, 3, 2):
            gather_wait(p, b, buf.at[chunk(0, lax.rem(z + 4 - k, 4))], k)

    def gather_out(b):
        first = c * 256 + b * 128

        def part_at(yy, k):
            return out_ref.at[chunk(first + yy * 64, lax.rem(z + 4 - k, 4))]

        def pass_on(part, s):
            start(part, part, cs_sem.at[b, s], cr_sem.at[b, s], quad[1])

        mine = part_at(y, 0)
        start(mine, mine, gys_sem.at[b, 0], gyr_sem.at[b, 0], quad[2])
        gather_start(2, b, mine)
        pass_on(mine, 0)
        yield
        for k in (1, 3, 2):
            part = part_at(y, k)
            gather_wait(2, b, part, k)
            start(part, part, gys_sem.at[b, k], gyr_sem.at[b, k], quad[2])
            pass_on(part, k)
        yield
        for k in (0, 1, 3, 2):
            part = part_at(1 - y, k)
            remote(part, part, gys_sem.at[b, k], gyr_sem.at[b, k], quad[2]).wait_recv()
            pass_on(part, 4 + k)

    def cross(half_id, b):
        lanes = span(half_id * 256 + b * 128, 128)
        q_blk = q_rcv[b, half_id].astype(F32).T

        def score_step(i, carry):
            rows = span(i * 8, 8)
            scores[rows, :] = jnp.sum(ck[rows, :, lanes].astype(F32) * q_blk[None], axis=1)
            return carry

        lax.fori_loop(0, 8, score_step, 0)
        s = scores[...] + jnp.where(mask_ref[:, lanes] != 0, 0.0, NEG_FILL)
        e = jnp.exp(s - jnp.max(s, axis=0, keepdims=True))
        scores[...] = (e / jnp.sum(e, axis=0, keepdims=True)).astype(BF16).astype(F32)

        def mix_step(i, acc):
            p_blk = scores[span(i * 8, 8), :]
            for j in range(8):
                acc = acc + cv[i * 8 + j, :, lanes].astype(F32) * p_blk[j:j + 1, :]
            return acc

        return lax.fori_loop(0, 8, mix_step, jnp.zeros((64, 128), F32)).T.astype(BF16)

    def flow(b):
        for r in (1, 2, 3):
            att[b, r].wait_recv()
        heads[b] = jnp.concatenate([attn_ref[rows_of(b, 0), :]] + [att_rcv[b, r] for r in range(3)], axis=1)
        if b == 0:
            once(local[2].wait, local[3].wait, *[copy.wait_recv for copy in wo_copies])
        partial = dot_nn(heads[b], wo4[...])
        total = yield from reduce_scatter(0, b, partial, (lambda: send_weight("cq", 3)) if b == 1 else None)
        local[b].wait()
        resid = x_buf[b].astype(F32) + total
        h_buf[0, b, chunk(0, z)] = rms_norm(resid, nc_ref[...])
        yield from gather(0, b)
        if b == 0:
            once(local[4].wait, *weight_waits("cq"))
        q4 = dot_nt(h_buf[0, b], cq4[...]).astype(BF16)
        for r in (3, 2, 1):
            q_snd[b, r - 1] = q4[:, r * 64:r * 64 + 64]
            start(q_snd.at[b, r - 1], q_rcv.at[b, c, span(y * 64, 64)], q_ssem.at[b, r - 1], q_rsem.at[b, r - 1], quad[r])
        q_rcv[b, c, span(y * 64, 64)] = q4[:, 0:64]
        if b == 0:
            send_weight("co", 3)
        else:
            for name in Y_SECOND:
                send_weight(name, 2)
        yield
        if b == 0:
            once(local[5].wait, local[6].wait)
        for half_id, pieces in ((c, (2,)), (1 - c, (1, 3))):
            for r in pieces:
                remote(q_snd.at[b, r - 1], q_rcv.at[b, quad_c[r], span(quad_y[r] * 64, 64)], q_ssem.at[b, r - 1], q_rsem.at[b, r - 1], quad[r]).wait_recv()
            o_buf[b, half_id] = cross(half_id, b)
            for r in reversed(pieces):
                start(o_buf.at[b, half_id, span(quad_y[r] * 64, 64)], o_rcv.at[b, r - 1], o_ssem.at[b, r - 1], o_rsem.at[b, r - 1], quad[r])
        if b == 1:
            for name in Y_THIRD:
                send_weight(name, 2)
            send_weight("wg", 3)
        yield
        for r in (1, 2, 3):
            remote(o_buf.at[b, quad_c[r], span(quad_y[r] * 64, 64)], o_rcv.at[b, r - 1], o_ssem.at[b, r - 1], o_rsem.at[b, r - 1], quad[r]).wait_recv()
        heads[b] = jnp.concatenate([o_buf[b, c, span(y * 64, 64), :]] + [o_rcv[b, r] for r in range(3)], axis=1)
        if b == 0:
            once(local[7].wait, *weight_waits("co"))
        partial = dot_nn(heads[b], co4[...])
        total = yield from reduce_scatter(1, b, partial, (lambda: send_weight("wu", 3)) if b == 1 else None)
        resid = resid + total
        h_buf[1, b, chunk(0, z)] = rms_norm(resid, nm_ref[...])
        yield from gather(1, b, (lambda: send_weight("wv", 3)) if b == 1 else None)
        if b == 0:
            send_weight("wd", 3)
            once(*[copy.wait for copy in local[8:]], *weight_waits("wg", "wu", "wv"))
        h = h_buf[1, b]
        act[b] = (gelu_tanh(dot_nt(h, wg4[...])) * dot_nt(h, wu4[...])).astype(BF16)
        if b == 0:
            once(*weight_waits("wd"))
        total = yield from reduce_scatter(2, b, dot_nn(act[b], wd4[...]))
        resid = resid + total
        out_ref[chunk(c * 256 + b * 128 + y * 64, z)] = resid.astype(BF16)
        yield from gather_out(b)

    flows = [flow(0), flow(1)]
    while flows:
        for item in list(flows):
            try:
                next(item)
            except StopIteration:
                flows.remove(item)
    for b in range(2):
        for s in range(8):
            yy = y if s < 4 else 1 - y
            part = out_ref.at[chunk((1 - c) * 256 + b * 128 + yy * 64, lax.rem(z + 4 - s % 4, 4))]
            remote(part, part, cs_sem.at[b, s], cr_sem.at[b, s], quad[1]).wait_recv()
    for copy in sends:
        copy.wait_send()


def tail(x_in, attn, mask_t, ck_t, cv_t, wo, cq_t, co, wg_t, wu_t, wd, woy, nc, nm):
    hbm = pl.BlockSpec(memory_space=pltpu.HBM)
    vmem = pl.BlockSpec(memory_space=pltpu.VMEM)
    units, wide = wd.shape
    deep = wo.shape[0]
    dma = pltpu.SemaphoreType.DMA
    bf16_shapes = [(2, 16, wide), ck_t.shape, cv_t.shape] + [(4 * deep, wide)] * 3 + [(4 * units, wide)] * 3
    bf16_shapes += [(2, 3, 64, deep), (2, 64, 4 * deep), (2, 3, 64, deep), (2, 2, 128, deep), (2, 2, 128, deep), (2, 3, 64, deep)]
    z_shapes = [(3, 2, 64, wide), (3, 2, 3, 16, wide), (2, 2, 64, wide), (2, 64, 4 * units)]
    sems = [(11,), (2,), (2,), (6, 3), (6, 3)] + [(2, 3)] * 6 + [(3, 2, 3)] * 4 + [(2, 4)] * 2 + [(2, 8)] * 2
    scratch = [pltpu.VMEM(shape, BF16) for shape in bf16_shapes]
    scratch += [pltpu.VMEM((deep, 128), F32), pltpu.VMEM((2, 64, wide), F32)]
    scratch += [pltpu.VMEM(shape, BF16) for shape in z_shapes] + [dma(shape) for shape in sems]
    return pl.pallas_call(
        tail_kernel,
        out_shape=jax.ShapeDtypeStruct(x_in.shape, BF16),
        in_specs=[hbm, vmem, vmem, hbm, hbm, vmem] + [hbm] * 6 + [vmem, vmem],
        out_specs=vmem,
        scratch_shapes=scratch,
        compiler_params=pltpu.CompilerParams(collective_id=0, has_side_effects=True, vmem_limit_bytes=50 * 2**20),
        name="tail",
    )(x_in, attn, mask_t, ck_t, cv_t, wo, cq_t, co, wg_t, wu_t, wd, woy, nc, nm)


def head_kernel(tok_ref, rb_ref, x_ref, wq_ref, wk_ref, wv_ref, ns_ref, k_hbm, v_hbm,
                attn_ref, nk_hbm, nv_hbm,
                kbuf, vbuf, h_buf, qq, k_new, v_new, table, in_sem, out_sem):
    rows, depth, t_len = kbuf.shape
    n_chunks = in_sem.shape[1]
    size = rows // n_chunks

    def chunk_copy(i, which):
        hbm, buf = ((k_hbm, kbuf), (v_hbm, vbuf))[which]
        part = pl.ds(i * size, size)
        return pltpu.make_async_copy(hbm.at[part], buf.at[part], in_sem.at[which, i])

    def chunk_out(i, which):
        hbm, buf = ((nk_hbm, kbuf), (nv_hbm, vbuf))[which]
        part = pl.ds(i * size, size)
        return pltpu.make_async_copy(buf.at[part], hbm.at[part], out_sem.at[which, i])

    for i in range(n_chunks):
        chunk_copy(i, 0).start()
        chunk_copy(i, 1).start()

    distance = lax.broadcasted_iota(jnp.int32, (t_len, t_len), 0) - lax.broadcasted_iota(jnp.int32, (t_len, t_len), 1)
    bias = jnp.full((t_len, t_len), rb_ref[0], F32)
    for bucket, edge in enumerate(BUCKET_EDGES):
        bias = jnp.where(distance >= edge, rb_ref[bucket + 1], bias)
    table[...] = jnp.where(distance >= 0, bias, NEG_FILL)

    wqq = jnp.concatenate([wq_ref[...], wq_ref[...]], axis=0)
    for i in range(rows // 128):
        part = slice(i * 128, i * 128 + 128)
        h = rms_norm(x_ref[part, :].astype(F32), ns_ref[...])
        qq[part, :] = dot_nt(h, wqq).astype(BF16).astype(F32)
        k_new[i] = dot_nt(wk_ref[...], h).astype(BF16).astype(F32)
        v_new[i] = dot_nt(wv_ref[...], h).astype(BF16).astype(F32)

    lane = lax.broadcasted_iota(jnp.int32, (depth, t_len), 1)
    row8 = lax.broadcasted_iota(jnp.int32, (8, 128), 0)
    half8 = lax.broadcasted_iota(jnp.int32, (8, 128), 1) // depth

    def step(i, carry):
        chunk_copy(i, 0).wait()
        chunk_copy(i, 1).wait()
        shift = lax.rem(i, 2) * size
        k_cols = pltpu.roll(k_new[i // 2], shift, 1)
        v_cols = pltpu.roll(v_new[i // 2], shift, 1)
        scores = []
        for g in range(size // 8):
            k8, bias8 = [], []
            for j in range(8):
                b = i * size + g * 8 + j
                pos = tok_ref[b]
                at_pos = lane == pos
                col = g * 8 + j
                k_b = jnp.where(at_pos, jnp.broadcast_to(k_cols[:, col:col + 1], (depth, t_len)), kbuf[b].astype(F32)).astype(BF16)
                v_b = jnp.where(at_pos, jnp.broadcast_to(v_cols[:, col:col + 1], (depth, t_len)), vbuf[b].astype(F32)).astype(BF16)
                kbuf[b] = k_b
                vbuf[b] = v_b
                k8.append(k_b)
                bias8.append(table[pl.ds(pos, 1), :])
            q8 = qq[pl.ds(pl.multiple_of(i * size + g * 8, 8), 8), :]
            q_diag = jnp.concatenate([jnp.where(row8 == 2 * m + half8, q8, 0.0) for m in range(4)], axis=1).astype(BF16)
            scores.append(dot_nn(q_diag, jnp.concatenate(k8, axis=0)) + jnp.concatenate(bias8, axis=0))
        chunk_out(i, 0).start()
        chunk_out(i, 1).start()
        s = jnp.concatenate(scores, axis=0)
        e = jnp.exp(s - jnp.max(s, axis=1, keepdims=True))
        p = (e / jnp.sum(e, axis=1, keepdims=True)).astype(BF16).astype(F32)
        outs = []
        for g in range(size // 8):
            p8 = p[g * 8:g * 8 + 8, :]
            p_diag = jnp.concatenate([jnp.where(row8 == j, p8, 0.0) for j in range(8)], axis=1).astype(BF16)
            v8 = jnp.concatenate([vbuf[i * size + g * 8 + j] for j in range(8)], axis=1)
            outs.append(dot_nt(p_diag, v8))
        attn_ref[pl.ds(pl.multiple_of(i * size, size), size), :] = jnp.concatenate(outs, axis=0).astype(BF16)
        return carry

    lax.fori_loop(0, n_chunks, step, 0)
    for i in range(n_chunks):
        chunk_out(i, 0).wait()
        chunk_out(i, 1).wait()


def head(tok_pos, rel_bias, x_in, wq_t, wk_t, wv_t, ns, k_t, v_t):
    hbm = pl.BlockSpec(memory_space=pltpu.HBM)
    vmem = pl.BlockSpec(memory_space=pltpu.VMEM)
    smem = pl.BlockSpec(memory_space=pltpu.SMEM)
    rows, depth, t_len = k_t.shape
    dma = pltpu.SemaphoreType.DMA
    n_chunks = 8
    return pl.pallas_call(
        head_kernel,
        out_shape=(jax.ShapeDtypeStruct((rows, depth), BF16), jax.ShapeDtypeStruct(k_t.shape, BF16), jax.ShapeDtypeStruct(v_t.shape, BF16)),
        in_specs=[smem, smem] + [vmem] * 5 + [hbm] * 2,
        out_specs=(vmem, hbm, hbm),
        scratch_shapes=[
            pltpu.VMEM(k_t.shape, BF16), pltpu.VMEM(v_t.shape, BF16), pltpu.VMEM((8, 128), BF16),
            pltpu.VMEM((rows, 2 * depth), F32), pltpu.VMEM((rows // 128, depth, 128), F32), pltpu.VMEM((rows // 128, depth, 128), F32),
            pltpu.VMEM((t_len, t_len), F32), dma((2, n_chunks)), dma((2, n_chunks)),
        ],
        compiler_params=pltpu.CompilerParams(vmem_limit_bytes=VMEM_BYTES),
        cost_estimate=pl.CostEstimate(flops=4 * 10**9, bytes_accessed=34 * 2**20, transcendentals=2**16),
        name="head",
    )(tok_pos, rel_bias, x_in, wq_t, wk_t, wv_t, ns, k_t, v_t)


def solution(mesh):
    def local_layer(x_in, tok_pos, self_k, self_v, cross_k, cross_v, enc_mask, rel_bias, w_q, w_k, w_v, w_o, cross_q, cross_o, w_gate, w_up, w_down, norm_self, norm_cross, norm_mlp):
        k_t = jnp.transpose(self_k[:, :, 0, :], (0, 2, 1))
        v_t = jnp.transpose(self_v[:, :, 0, :], (0, 2, 1))
        attn, new_k, new_v = head(tok_pos, rel_bias[:, 0], x_in, w_q.T, w_k.T, w_v.T, norm_self, k_t, v_t)
        new_self_k = jnp.transpose(new_k, (0, 2, 1))[:, :, None, :]
        new_self_v = jnp.transpose(new_v, (0, 2, 1))[:, :, None, :]
        ck_t = jnp.transpose(cross_k[:, :, 0, :], (1, 2, 0))
        cv_t = jnp.transpose(cross_v[:, :, 0, :], (1, 2, 0))
        wo_y = lax.ppermute(w_o, "tp", [(i, i ^ 2) for i in range(mesh.shape["tp"])])
        out = tail(x_in, attn, enc_mask.T, ck_t, cv_t, w_o, cross_q.T, cross_o, w_gate.T, w_up.T, w_down, wo_y, norm_cross, norm_mlp)
        return out, new_self_k, new_self_v

    cache_spec = P('dp', None, 'tp', None)
    split_cols = P(None, 'tp')
    split_rows = P('tp', None)
    in_specs = (P('dp', None), P('dp'), cache_spec, cache_spec, cache_spec, cache_spec, P('dp', None), split_cols, split_cols, split_cols, split_cols, split_rows, split_cols, split_rows, split_cols, split_cols, split_rows, P(None), P(None), P(None))
    out_specs = (P('dp', None), cache_spec, cache_spec)
    return jax.shard_map(local_layer, mesh=mesh, in_specs=in_specs, out_specs=out_specs, check_vma=False)
```

```python
import math
import jax
import jax.numpy as jnp
from jax import lax
from jax.experimental import pallas as pl
from jax.experimental.pallas import tpu as pltpu
from jax.sharding import PartitionSpec as P

BUCKET_EDGES = tuple(range(1, 16)) + (16,) + tuple(int(math.ceil(16.0 * 8.0 ** (m / 16.0))) for m in range(1, 16))
NEG_FILL = -1e30
MESH = pl.DeviceIdType.MESH
F32 = jnp.float32
BF16 = jnp.bfloat16
K_ORDER = (3, 2, 1)
Y_FIRST, Y_SECOND, Y_THIRD = ("cq", "co", "wg"), ("wu",), ("wv", "wd")
VMEM_BYTES = 60 * 1024 * 1024


def rms_norm(values, norm_scale):
    inv_rms = lax.rsqrt(jnp.mean(values * values, axis=-1, keepdims=True) + 1e-6)
    return (values * inv_rms * norm_scale.astype(F32)[None, :]).astype(BF16)


def gelu_tanh(u):
    return u * (0.5 * (1.0 + jnp.tanh(math.sqrt(2.0 / math.pi) * (u + 0.044715 * (u * u * u)))))


def dot_nt(a, b):
    return lax.dot_general(a, b, (((1,), (1,)), ((), ())), preferred_element_type=F32)


def dot_nn(a, b):
    return jnp.dot(a, b, preferred_element_type=F32)


def tail_kernel(x_hbm, attn_ref, mask_ref, ck_hbm, cv_hbm, wo_ref, cq_hbm, co_hbm, wg_hbm, wu_hbm, wd_hbm, woy_hbm, nc_ref, nm_ref,
                out_ref,
                x_buf, ck, cv, wo4, cq4, co4, wg4, wu4, wd4, att_rcv, heads, q_snd, q_rcv, o_buf, o_rcv, scores,
                own, z_snd, z_rcv, h_buf, act,
                loc_sem, wo_ssem, wo_rsem, w_ssem, w_rsem, at_ssem, at_rsem, q_ssem, q_rsem, o_ssem, o_rsem, zs_sem, zr_sem, gzs_sem, gzr_sem, gys_sem, gyr_sem, cs_sem, cr_sem):
    me = lax.axis_index("tp")
    c = lax.rem(me, 2)
    y = lax.rem(me // 2, 2)
    z = me // 4
    quad = {r: {"tp": z * 4 + (y if r < 2 else 1 - y) * 2 + (c if r == 2 else 1 - c)} for r in (1, 2, 3)}
    quad_c = {0: c, 1: 1 - c, 2: c, 3: 1 - c}
    quad_y = {0: y, 1: y, 2: 1 - y, 3: 1 - y}
    z_peer = {k: {"tp": lax.rem(z + k, 4) * 4 + y * 2 + c} for k in (1, 2, 3)}
    sends = []

    def remote(src, dst, ssem, rsem, peer):
        return pltpu.make_async_remote_copy(src_ref=src, dst_ref=dst, send_sem=ssem, recv_sem=rsem, device_id=peer, device_id_type=MESH)

    def start(src, dst, ssem, rsem, peer):
        copy = remote(src, dst, ssem, rsem, peer)
        copy.start()
        sends.append(copy)
        return copy

    def span(base, size):
        return pl.ds(pl.multiple_of(base, size), size)

    def chunk(base, zz):
        return span(base + zz * 16, 16)

    def slot(ref, r):
        size = ref.shape[0] // 4
        return ref.at[pl.ds(r * size, size)]

    local = [pltpu.make_async_copy(src, dst, loc_sem.at[i]) for i, (src, dst) in enumerate((
        (x_hbm.at[chunk(c * 256 + y * 64, z)], x_buf.at[0]),
        (x_hbm.at[chunk(c * 256 + 128 + y * 64, z)], x_buf.at[1]),
        (wo_ref, slot(wo4, 0)), (woy_hbm, slot(wo4, 2)), (cq_hbm, slot(cq4, 0)), (ck_hbm, ck), (cv_hbm, cv), (co_hbm, slot(co4, 0)),
        (wg_hbm, slot(wg4, 0)), (wu_hbm, slot(wu4, 0)), (wd_hbm, slot(wd4, 0)),
    ))]
    for copy in local:
        copy.start()

    barrier = pltpu.get_barrier_semaphore()
    for peer in (quad[1], quad[2], quad[3], z_peer[1], z_peer[2], z_peer[3]):
        pl.semaphore_signal(barrier, inc=1, device_id=peer, device_id_type=MESH)
    pl.semaphore_wait(barrier, 6)

    def rows_of(b, r):
        return span(quad_c[r] * 256 + b * 128 + quad_y[r] * 64, 64)

    att = {}
    for b in range(2):
        for r in (3, 2, 1):
            att[b, r] = start(attn_ref.at[rows_of(b, r)], att_rcv.at[b, r - 1], at_ssem.at[b, r - 1], at_rsem.at[b, r - 1], quad[r])
    part = 96
    pieces = {
        "cq": (cq_hbm, cq4, 0, cq_hbm.shape[0]), "co": (co_hbm, co4, 0, co_hbm.shape[0]),
        "wg": (wg_hbm, wg4, 0, wg_hbm.shape[0]), "wu": (wu_hbm, wu4, 0, part), "wv": (wu_hbm, wu4, part, wu_hbm.shape[0] - part),
        "wd": (wd_hbm, wd4, 0, wd_hbm.shape[0]),
    }
    w_copy = {}

    def send_weight(name, r):
        src, slots, first, size = pieces[name]
        rows = pl.ds(first, size)
        if r == 3:
            w_copy[name, 2].wait_recv()
            src = slot(slots, 2)
        i = list(pieces).index(name)
        w_copy[name, r] = start(src.at[rows], slot(slots, r).at[rows], w_ssem.at[i, r - 1], w_rsem.at[i, r - 1], quad[2 if r == 2 else 1])

    def weight_waits(*names):
        return [w_copy[name, r].wait_recv for name in names for r in (1, 3)]

    wo_copies = [start(src, slot(wo4, r), wo_ssem.at[r // 2], wo_rsem.at[r // 2], quad[1]) for src, r in ((wo_ref, 1), (woy_hbm, 3))]
    for name in pieces:
        send_weight(name, 1)
    for name in Y_FIRST:
        send_weight(name, 2)

    def once(*waits):
        for wait in waits:
            wait()

    def reduce_scatter(p, b, partial, then=None):
        own[b] = partial
        z_snd[p, b] = partial.astype(BF16)
        copies = {}
        for k in K_ORDER:
            copies[k] = start(z_snd.at[p, b, chunk(0, lax.rem(z + k, 4))], z_rcv.at[p, b, k - 1], zs_sem.at[p, b, k - 1], zr_sem.at[p, b, k - 1], z_peer[k])
        if then is not None:
            then()
        yield
        total = own[b, chunk(0, z)]
        for k in (1, 3, 2):
            copies[k].wait_recv()
            total = total + z_rcv[p, b, k - 1].astype(F32)
        return total

    def gather_start(p, b, mine):
        for k in K_ORDER:
            start(mine, mine, gzs_sem.at[p, b, k - 1], gzr_sem.at[p, b, k - 1], z_peer[k])

    def gather_wait(p, b, part, k):
        remote(part, part, gzs_sem.at[p, b, k - 1], gzr_sem.at[p, b, k - 1], z_peer[k]).wait_recv()

    def gather(p, b, then=None):
        buf = h_buf.at[p, b]
        gather_start(p, b, buf.at[chunk(0, z)])
        if then is not None:
            then()
        yield
        for k in (1, 3, 2):
            gather_wait(p, b, buf.at[chunk(0, lax.rem(z + 4 - k, 4))], k)

    def gather_out(b):
        first = c * 256 + b * 128

        def part_at(yy, k):
            return out_ref.at[chunk(first + yy * 64, lax.rem(z + 4 - k, 4))]

        def pass_on(part, s):
            start(part, part, cs_sem.at[b, s], cr_sem.at[b, s], quad[1])

        mine = part_at(y, 0)
        start(mine, mine, gys_sem.at[b, 0], gyr_sem.at[b, 0], quad[2])
        gather_start(2, b, mine)
        pass_on(mine, 0)
        yield
        for k in (1, 3, 2):
            part = part_at(y, k)
            gather_wait(2, b, part, k)
            start(part, part, gys_sem.at[b, k], gyr_sem.at[b, k], quad[2])
            pass_on(part, k)
        yield
        for k in (0, 1, 3, 2):
            part = part_at(1 - y, k)
            remote(part, part, gys_sem.at[b, k], gyr_sem.at[b, k], quad[2]).wait_recv()
            pass_on(part, 4 + k)

    def cross(half_id, b):
        lanes = span(half_id * 256 + b * 128, 128)
        q_blk = q_rcv[b, half_id].astype(F32).T

        def score_step(i, carry):
            rows = span(i * 8, 8)
            scores[rows, :] = jnp.sum(ck[rows, :, lanes].astype(F32) * q_blk[None], axis=1)
            return carry

        lax.fori_loop(0, 8, score_step, 0)
        s = scores[...] + jnp.where(mask_ref[:, lanes] != 0, 0.0, NEG_FILL)
        e = jnp.exp(s - jnp.max(s, axis=0, keepdims=True))
        scores[...] = (e / jnp.sum(e, axis=0, keepdims=True)).astype(BF16).astype(F32)

        def mix_step(i, acc):
            p_blk = scores[span(i * 8, 8), :]
            for j in range(8):
                acc = acc + cv[i * 8 + j, :, lanes].astype(F32) * p_blk[j:j + 1, :]
            return acc

        return lax.fori_loop(0, 8, mix_step, jnp.zeros((64, 128), F32)).T.astype(BF16)

    def flow(b):
        for r in (1, 2, 3):
            att[b, r].wait_recv()
        heads[b] = jnp.concatenate([attn_ref[rows_of(b, 0), :]] + [att_rcv[b, r] for r in range(3)], axis=1)
        if b == 0:
            once(local[2].wait, local[3].wait, *[copy.wait_recv for copy in wo_copies])
        partial = dot_nn(heads[b], wo4[...])
        total = yield from reduce_scatter(0, b, partial, (lambda: send_weight("cq", 3)) if b == 1 else None)
        local[b].wait()
        resid = x_buf[b].astype(F32) + total
        h_buf[0, b, chunk(0, z)] = rms_norm(resid, nc_ref[...])
        yield from gather(0, b)
        if b == 0:
            once(local[4].wait, *weight_waits("cq"))
        q4 = dot_nt(h_buf[0, b], cq4[...]).astype(BF16)
        for r in (3, 2, 1):
            q_snd[b, r - 1] = q4[:, r * 64:r * 64 + 64]
            start(q_snd.at[b, r - 1], q_rcv.at[b, c, span(y * 64, 64)], q_ssem.at[b, r - 1], q_rsem.at[b, r - 1], quad[r])
        q_rcv[b, c, span(y * 64, 64)] = q4[:, 0:64]
        if b == 0:
            send_weight("co", 3)
        else:
            for name in Y_SECOND:
                send_weight(name, 2)
        yield
        if b == 0:
            once(local[5].wait, local[6].wait)
        for half_id, pieces in ((c, (2,)), (1 - c, (1, 3))):
            for r in pieces:
                remote(q_snd.at[b, r - 1], q_rcv.at[b, quad_c[r], span(quad_y[r] * 64, 64)], q_ssem.at[b, r - 1], q_rsem.at[b, r - 1], quad[r]).wait_recv()
            o_buf[b, half_id] = cross(half_id, b)
            for r in reversed(pieces):
                start(o_buf.at[b, half_id, span(quad_y[r] * 64, 64)], o_rcv.at[b, r - 1], o_ssem.at[b, r - 1], o_rsem.at[b, r - 1], quad[r])
        if b == 1:
            for name in Y_THIRD:
                send_weight(name, 2)
            send_weight("wg", 3)
        yield
        for r in (1, 2, 3):
            remote(o_buf.at[b, quad_c[r], span(quad_y[r] * 64, 64)], o_rcv.at[b, r - 1], o_ssem.at[b, r - 1], o_rsem.at[b, r - 1], quad[r]).wait_recv()
        heads[b] = jnp.concatenate([o_buf[b, c, span(y * 64, 64), :]] + [o_rcv[b, r] for r in range(3)], axis=1)
        if b == 0:
            once(local[7].wait, *weight_waits("co"))
        partial = dot_nn(heads[b], co4[...])
        total = yield from reduce_scatter(1, b, partial, (lambda: send_weight("wu", 3)) if b == 1 else None)
        resid = resid + total
        h_buf[1, b, chunk(0, z)] = rms_norm(resid, nm_ref[...])
        yield from gather(1, b, (lambda: send_weight("wv", 3)) if b == 1 else None)
        if b == 0:
            send_weight("wd", 3)
            once(*[copy.wait for copy in local[8:]], *weight_waits("wg", "wu", "wv"))
        h = h_buf[1, b]
        act[b] = (gelu_tanh(dot_nt(h, wg4[...])) * dot_nt(h, wu4[...])).astype(BF16)
        if b == 0:
            once(*weight_waits("wd"))
        total = yield from reduce_scatter(2, b, dot_nn(act[b], wd4[...]))
        resid = resid + total
        out_ref[chunk(c * 256 + b * 128 + y * 64, z)] = resid.astype(BF16)
        yield from gather_out(b)

    flows = [flow(0), flow(1)]
    while flows:
        for item in list(flows):
            try:
                next(item)
            except StopIteration:
                flows.remove(item)
    for b in range(2):
        for s in range(8):
            yy = y if s < 4 else 1 - y
            part = out_ref.at[chunk((1 - c) * 256 + b * 128 + yy * 64, lax.rem(z + 4 - s % 4, 4))]
            remote(part, part, cs_sem.at[b, s], cr_sem.at[b, s], quad[1]).wait_recv()
    for copy in sends:
        copy.wait_send()


def tail(x_in, attn, mask_t, ck_t, cv_t, wo, cq_t, co, wg_t, wu_t, wd, woy, nc, nm):
    hbm = pl.BlockSpec(memory_space=pltpu.HBM)
    vmem = pl.BlockSpec(memory_space=pltpu.VMEM)
    units, wide = wd.shape
    deep = wo.shape[0]
    dma = pltpu.SemaphoreType.DMA
    bf16_shapes = [(2, 16, wide), ck_t.shape, cv_t.shape] + [(4 * deep, wide)] * 3 + [(4 * units, wide)] * 3
    bf16_shapes += [(2, 3, 64, deep), (2, 64, 4 * deep), (2, 3, 64, deep), (2, 2, 128, deep), (2, 2, 128, deep), (2, 3, 64, deep)]
    z_shapes = [(3, 2, 64, wide), (3, 2, 3, 16, wide), (2, 2, 64, wide), (2, 64, 4 * units)]
    sems = [(11,), (2,), (2,), (6, 3), (6, 3)] + [(2, 3)] * 6 + [(3, 2, 3)] * 4 + [(2, 4)] * 2 + [(2, 8)] * 2
    scratch = [pltpu.VMEM(shape, BF16) for shape in bf16_shapes]
    scratch += [pltpu.VMEM((deep, 128), F32), pltpu.VMEM((2, 64, wide), F32)]
    scratch += [pltpu.VMEM(shape, BF16) for shape in z_shapes] + [dma(shape) for shape in sems]
    return pl.pallas_call(
        tail_kernel,
        out_shape=jax.ShapeDtypeStruct(x_in.shape, BF16),
        in_specs=[hbm, vmem, vmem, hbm, hbm, vmem] + [hbm] * 6 + [vmem, vmem],
        out_specs=vmem,
        scratch_shapes=scratch,
        compiler_params=pltpu.CompilerParams(collective_id=0, has_side_effects=True, vmem_limit_bytes=50 * 2**20),
        name="tail",
    )(x_in, attn, mask_t, ck_t, cv_t, wo, cq_t, co, wg_t, wu_t, wd, woy, nc, nm)


def head_kernel(tok_ref, rb_ref, x_ref, wq_ref, wk_ref, wv_ref, ns_ref, k_hbm, v_hbm,
                attn_ref, nk_hbm, nv_hbm,
                kbuf, vbuf, h_buf, qq, k_new, v_new, table, in_sem, out_sem):
    rows, depth, t_len = kbuf.shape
    n_chunks = in_sem.shape[1]
    size = rows // n_chunks

    def chunk_copy(i, which):
        hbm, buf = ((k_hbm, kbuf), (v_hbm, vbuf))[which]
        part = pl.ds(i * size, size)
        return pltpu.make_async_copy(hbm.at[part], buf.at[part], in_sem.at[which, i])

    def chunk_out(i, which):
        hbm, buf = ((nk_hbm, kbuf), (nv_hbm, vbuf))[which]
        part = pl.ds(i * size, size)
        return pltpu.make_async_copy(buf.at[part], hbm.at[part], out_sem.at[which, i])

    for i in range(n_chunks):
        chunk_copy(i, 0).start()
        chunk_copy(i, 1).start()

    distance = lax.broadcasted_iota(jnp.int32, (t_len, t_len), 0) - lax.broadcasted_iota(jnp.int32, (t_len, t_len), 1)
    bias = jnp.full((t_len, t_len), rb_ref[0], F32)
    for bucket, edge in enumerate(BUCKET_EDGES):
        bias = jnp.where(distance >= edge, rb_ref[bucket + 1], bias)
    table[...] = jnp.where(distance >= 0, bias, NEG_FILL)

    wqq = jnp.concatenate([wq_ref[...], wq_ref[...]], axis=0)
    for i in range(rows // 128):
        part = slice(i * 128, i * 128 + 128)
        h = rms_norm(x_ref[part, :].astype(F32), ns_ref[...])
        qq[part, :] = dot_nt(h, wqq).astype(BF16).astype(F32)
        k_new[i] = dot_nt(wk_ref[...], h).astype(BF16).astype(F32)
        v_new[i] = dot_nt(wv_ref[...], h).astype(BF16).astype(F32)

    lane = lax.broadcasted_iota(jnp.int32, (depth, t_len), 1)
    row8 = lax.broadcasted_iota(jnp.int32, (8, 128), 0)
    half8 = lax.broadcasted_iota(jnp.int32, (8, 128), 1) // depth

    def step(i, carry):
        chunk_copy(i, 0).wait()
        chunk_copy(i, 1).wait()
        k_cols, v_cols = k_new[i], v_new[i]
        scores = []
        for g in range(size // 8):
            k8, bias8 = [], []
            for j in range(8):
                b = i * size + g * 8 + j
                pos = tok_ref[b]
                at_pos = lane == pos
                col = g * 8 + j
                k_b = jnp.where(at_pos, pltpu.roll(k_cols, pos + (t_len - col), 1), kbuf[b].astype(F32)).astype(BF16)
                v_b = jnp.where(at_pos, pltpu.roll(v_cols, pos + (t_len - col), 1), vbuf[b].astype(F32)).astype(BF16)
                kbuf[b] = k_b
                vbuf[b] = v_b
                k8.append(k_b)
                bias8.append(table[pl.ds(pos, 1), :])
            q8 = qq[pl.ds(pl.multiple_of(i * size + g * 8, 8), 8), :]
            q_diag = jnp.concatenate([jnp.where(row8 == 2 * m + half8, q8, 0.0) for m in range(4)], axis=1).astype(BF16)
            scores.append(dot_nn(q_diag, jnp.concatenate(k8, axis=0)) + jnp.concatenate(bias8, axis=0))
        chunk_out(i, 0).start()
        chunk_out(i, 1).start()
        s = jnp.concatenate(scores, axis=0)
        e = jnp.exp(s - jnp.max(s, axis=1, keepdims=True))
        p = (e / jnp.sum(e, axis=1, keepdims=True)).astype(BF16).astype(F32)
        outs = []
        for g in range(size // 8):
            p8 = p[g * 8:g * 8 + 8, :]
            p_diag = jnp.concatenate([jnp.where(row8 == j, p8, 0.0) for j in range(8)], axis=1).astype(BF16)
            v8 = jnp.concatenate([vbuf[i * size + g * 8 + j] for j in range(8)], axis=1)
            outs.append(dot_nt(p_diag, v8))
        attn_ref[pl.ds(pl.multiple_of(i * size, size), size), :] = jnp.concatenate(outs, axis=0).astype(BF16)
        return carry

    lax.fori_loop(0, n_chunks, step, 0)
    for i in range(n_chunks):
        chunk_out(i, 0).wait()
        chunk_out(i, 1).wait()


def head(tok_pos, rel_bias, x_in, wq_t, wk_t, wv_t, ns, k_t, v_t):
    hbm = pl.BlockSpec(memory_space=pltpu.HBM)
    vmem = pl.BlockSpec(memory_space=pltpu.VMEM)
    smem = pl.BlockSpec(memory_space=pltpu.SMEM)
    rows, depth, t_len = k_t.shape
    dma = pltpu.SemaphoreType.DMA
    n_chunks = 4
    return pl.pallas_call(
        head_kernel,
        out_shape=(jax.ShapeDtypeStruct((rows, depth), BF16), jax.ShapeDtypeStruct(k_t.shape, BF16), jax.ShapeDtypeStruct(v_t.shape, BF16)),
        in_specs=[smem, smem] + [vmem] * 5 + [hbm] * 2,
        out_specs=(vmem, hbm, hbm),
        scratch_shapes=[
            pltpu.VMEM(k_t.shape, BF16), pltpu.VMEM(v_t.shape, BF16), pltpu.VMEM((8, 128), BF16),
            pltpu.VMEM((rows, 2 * depth), F32), pltpu.VMEM((rows // 128, depth, 128), F32), pltpu.VMEM((rows // 128, depth, 128), F32),
            pltpu.VMEM((t_len, t_len), F32), dma((2, n_chunks)), dma((2, n_chunks)),
        ],
        compiler_params=pltpu.CompilerParams(vmem_limit_bytes=VMEM_BYTES),
        cost_estimate=pl.CostEstimate(flops=4 * 10**9, bytes_accessed=34 * 2**20, transcendentals=2**16),
        name="head",
    )(tok_pos, rel_bias, x_in, wq_t, wk_t, wv_t, ns, k_t, v_t)


def solution(mesh):
    def local_layer(x_in, tok_pos, self_k, self_v, cross_k, cross_v, enc_mask, rel_bias, w_q, w_k, w_v, w_o, cross_q, cross_o, w_gate, w_up, w_down, norm_self, norm_cross, norm_mlp):
        k_t = jnp.transpose(self_k[:, :, 0, :], (0, 2, 1))
        v_t = jnp.transpose(self_v[:, :, 0, :], (0, 2, 1))
        attn, new_k, new_v = head(tok_pos, rel_bias[:, 0], x_in, w_q.T, w_k.T, w_v.T, norm_self, k_t, v_t)
        new_self_k = jnp.transpose(new_k, (0, 2, 1))[:, :, None, :]
        new_self_v = jnp.transpose(new_v, (0, 2, 1))[:, :, None, :]
        ck_t = jnp.transpose(cross_k[:, :, 0, :], (1, 2, 0))
        cv_t = jnp.transpose(cross_v[:, :, 0, :], (1, 2, 0))
        wo_y = lax.ppermute(w_o, "tp", [(i, i ^ 2) for i in range(mesh.shape["tp"])])
        out = tail(x_in, attn, enc_mask.T, ck_t, cv_t, w_o, cross_q.T, cross_o, w_gate.T, w_up.T, w_down, wo_y, norm_cross, norm_mlp)
        return out, new_self_k, new_self_v

    cache_spec = P('dp', None, 'tp', None)
    split_cols = P(None, 'tp')
    split_rows = P('tp', None)
    in_specs = (P('dp', None), P('dp'), cache_spec, cache_spec, cache_spec, cache_spec, P('dp', None), split_cols, split_cols, split_cols, split_cols, split_rows, split_cols, split_rows, split_cols, split_cols, split_rows, P(None), P(None), P(None))
    out_specs = (P('dp', None), cache_spec, cache_spec)
    return jax.shard_map(local_layer, mesh=mesh, in_specs=in_specs, out_specs=out_specs, check_vma=False)
```

```python
import math
import jax
import jax.numpy as jnp
from jax import lax
from jax.experimental import pallas as pl
from jax.experimental.pallas import tpu as pltpu
from jax.sharding import PartitionSpec as P

BUCKET_EDGES = tuple(range(1, 16)) + (16,) + tuple(int(math.ceil(16.0 * 8.0 ** (m / 16.0))) for m in range(1, 16))
NEG_FILL = -1e30
MESH = pl.DeviceIdType.MESH
F32 = jnp.float32
BF16 = jnp.bfloat16
K_ORDER = (3, 2, 1)
Y_FIRST, Y_SECOND, Y_THIRD = ("cq", "co", "wg"), ("wu",), ("wv", "wd")
VMEM_BYTES = 60 * 1024 * 1024


def rms_norm(values, norm_scale):
    inv_rms = lax.rsqrt(jnp.mean(values * values, axis=-1, keepdims=True) + 1e-6)
    return (values * inv_rms * norm_scale.astype(F32)[None, :]).astype(BF16)


def gelu_tanh(u):
    return u * (0.5 * (1.0 + jnp.tanh(math.sqrt(2.0 / math.pi) * (u + 0.044715 * (u * u * u)))))


def dot_nt(a, b):
    return lax.dot_general(a, b, (((1,), (1,)), ((), ())), preferred_element_type=F32)


def dot_nn(a, b):
    return jnp.dot(a, b, preferred_element_type=F32)


def tail_kernel(x_hbm, attn_ref, mask_ref, ck_hbm, cv_hbm, wo_ref, cq_hbm, co_hbm, wg_hbm, wu_hbm, wd_hbm, woy_hbm, nc_ref, nm_ref,
                out_ref,
                x_buf, ck, cv, wo4, cq4, co4, wg4, wu4, wd4, att_rcv, heads, q_snd, q_rcv, o_buf, o_rcv, scores,
                own, z_snd, z_rcv, h_buf, act,
                loc_sem, wo_ssem, wo_rsem, w_ssem, w_rsem, at_ssem, at_rsem, q_ssem, q_rsem, o_ssem, o_rsem, zs_sem, zr_sem, gzs_sem, gzr_sem, gys_sem, gyr_sem, cs_sem, cr_sem):
    me = lax.axis_index("tp")
    c = lax.rem(me, 2)
    y = lax.rem(me // 2, 2)
    z = me // 4
    quad = {r: {"tp": z * 4 + (y if r < 2 else 1 - y) * 2 + (c if r == 2 else 1 - c)} for r in (1, 2, 3)}
    quad_c = {0: c, 1: 1 - c, 2: c, 3: 1 - c}
    quad_y = {0: y, 1: y, 2: 1 - y, 3: 1 - y}
    z_peer = {k: {"tp": lax.rem(z + k, 4) * 4 + y * 2 + c} for k in (1, 2, 3)}
    sends = []

    def remote(src, dst, ssem, rsem, peer):
        return pltpu.make_async_remote_copy(src_ref=src, dst_ref=dst, send_sem=ssem, recv_sem=rsem, device_id=peer, device_id_type=MESH)

    def start(src, dst, ssem, rsem, peer):
        copy = remote(src, dst, ssem, rsem, peer)
        copy.start()
        sends.append(copy)
        return copy

    def span(base, size):
        return pl.ds(pl.multiple_of(base, size), size)

    def chunk(base, zz):
        return span(base + zz * 16, 16)

    def slot(ref, r):
        size = ref.shape[0] // 4
        return ref.at[pl.ds(r * size, size)]

    local = [pltpu.make_async_copy(src, dst, loc_sem.at[i]) for i, (src, dst) in enumerate((
        (x_hbm.at[chunk(c * 256 + y * 64, z)], x_buf.at[0]),
        (x_hbm.at[chunk(c * 256 + 128 + y * 64, z)], x_buf.at[1]),
        (wo_ref, slot(wo4, 0)), (woy_hbm, slot(wo4, 2)), (cq_hbm, slot(cq4, 0)), (ck_hbm, ck), (cv_hbm, cv), (co_hbm, slot(co4, 0)),
        (wg_hbm, slot(wg4, 0)), (wu_hbm, slot(wu4, 0)), (wd_hbm, slot(wd4, 0)),
    ))]
    for copy in local:
        copy.start()

    barrier = pltpu.get_barrier_semaphore()
    for peer in (quad[1], quad[2], quad[3], z_peer[1], z_peer[2], z_peer[3]):
        pl.semaphore_signal(barrier, inc=1, device_id=peer, device_id_type=MESH)
    pl.semaphore_wait(barrier, 6)

    def rows_of(b, r):
        return span(quad_c[r] * 256 + b * 128 + quad_y[r] * 64, 64)

    att = {}
    for b in range(2):
        for r in (3, 2, 1):
            att[b, r] = start(attn_ref.at[rows_of(b, r)], att_rcv.at[b, r - 1], at_ssem.at[b, r - 1], at_rsem.at[b, r - 1], quad[r])
    part = 96
    pieces = {
        "cq": (cq_hbm, cq4, 0, cq_hbm.shape[0]), "co": (co_hbm, co4, 0, co_hbm.shape[0]),
        "wg": (wg_hbm, wg4, 0, wg_hbm.shape[0]), "wu": (wu_hbm, wu4, 0, part), "wv": (wu_hbm, wu4, part, wu_hbm.shape[0] - part),
        "wd": (wd_hbm, wd4, 0, wd_hbm.shape[0]),
    }
    w_copy = {}

    def send_weight(name, r):
        src, slots, first, size = pieces[name]
        rows = pl.ds(first, size)
        if r == 3:
            w_copy[name, 2].wait_recv()
            src = slot(slots, 2)
        i = list(pieces).index(name)
        w_copy[name, r] = start(src.at[rows], slot(slots, r).at[rows], w_ssem.at[i, r - 1], w_rsem.at[i, r - 1], quad[2 if r == 2 else 1])

    def weight_waits(*names):
        return [w_copy[name, r].wait_recv for name in names for r in (1, 3)]

    wo_copies = [start(src, slot(wo4, r), wo_ssem.at[r // 2], wo_rsem.at[r // 2], quad[1]) for src, r in ((wo_ref, 1), (woy_hbm, 3))]
    for name in pieces:
        send_weight(name, 1)
    for name in Y_FIRST:
        send_weight(name, 2)

    def once(*waits):
        for wait in waits:
            wait()

    def reduce_scatter(p, b, partial, then=None):
        own[b] = partial
        z_snd[p, b] = partial.astype(BF16)
        copies = {}
        for k in K_ORDER:
            copies[k] = start(z_snd.at[p, b, chunk(0, lax.rem(z + k, 4))], z_rcv.at[p, b, k - 1], zs_sem.at[p, b, k - 1], zr_sem.at[p, b, k - 1], z_peer[k])
        if then is not None:
            then()
        yield
        total = own[b, chunk(0, z)]
        for k in (1, 3, 2):
            copies[k].wait_recv()
            total = total + z_rcv[p, b, k - 1].astype(F32)
        return total

    def gather_start(p, b, mine):
        for k in (2, 1, 3):
            start(mine, mine, gzs_sem.at[p, b, k - 1], gzr_sem.at[p, b, k - 1], z_peer[k])

    def gather_wait(p, b, part, k):
        remote(part, part, gzs_sem.at[p, b, k - 1], gzr_sem.at[p, b, k - 1], z_peer[k]).wait_recv()

    def gather(p, b, then=None):
        buf = h_buf.at[p, b]
        gather_start(p, b, buf.at[chunk(0, z)])
        if then is not None:
            then()
        yield
        for k in (1, 3, 2):
            gather_wait(p, b, buf.at[chunk(0, lax.rem(z + 4 - k, 4))], k)

    def gather_out(b):
        first = c * 256 + b * 128

        def part_at(yy, k):
            return out_ref.at[chunk(first + yy * 64, lax.rem(z + 4 - k, 4))]

        def pass_on(part, s):
            start(part, part, cs_sem.at[b, s], cr_sem.at[b, s], quad[1])

        mine = part_at(y, 0)
        start(mine, mine, gys_sem.at[b, 0], gyr_sem.at[b, 0], quad[2])
        gather_start(2, b, mine)
        pass_on(mine, 0)
        yield
        for k in (1, 3, 2):
            part = part_at(y, k)
            gather_wait(2, b, part, k)
            start(part, part, gys_sem.at[b, k], gyr_sem.at[b, k], quad[2])
            pass_on(part, k)
        yield
        for k in (0, 1, 3, 2):
            part = part_at(1 - y, k)
            remote(part, part, gys_sem.at[b, k], gyr_sem.at[b, k], quad[2]).wait_recv()
            pass_on(part, 4 + k)

    def cross(half_id, b):
        lanes = span(half_id * 256 + b * 128, 128)
        q_blk = q_rcv[b, half_id].astype(F32).T

        def score_step(i, carry):
            rows = span(i * 8, 8)
            scores[rows, :] = jnp.sum(ck[rows, :, lanes].astype(F32) * q_blk[None], axis=1)
            return carry

        lax.fori_loop(0, 8, score_step, 0)
        s = scores[...] + jnp.where(mask_ref[:, lanes] != 0, 0.0, NEG_FILL)
        e = jnp.exp(s - jnp.max(s, axis=0, keepdims=True))
        scores[...] = (e / jnp.sum(e, axis=0, keepdims=True)).astype(BF16).astype(F32)

        def mix_step(i, acc):
            p_blk = scores[span(i * 8, 8), :]
            for j in range(8):
                acc = acc + cv[i * 8 + j, :, lanes].astype(F32) * p_blk[j:j + 1, :]
            return acc

        return lax.fori_loop(0, 8, mix_step, jnp.zeros((64, 128), F32)).T.astype(BF16)

    def flow(b):
        for r in (1, 2, 3):
            att[b, r].wait_recv()
        heads[b] = jnp.concatenate([attn_ref[rows_of(b, 0), :]] + [att_rcv[b, r] for r in range(3)], axis=1)
        if b == 0:
            once(local[2].wait, local[3].wait, *[copy.wait_recv for copy in wo_copies])
        partial = dot_nn(heads[b], wo4[...])
        total = yield from reduce_scatter(0, b, partial, (lambda: send_weight("cq", 3)) if b == 1 else None)
        local[b].wait()
        resid = x_buf[b].astype(F32) + total
        h_buf[0, b, chunk(0, z)] = rms_norm(resid, nc_ref[...])
        yield from gather(0, b)
        if b == 0:
            once(local[4].wait, *weight_waits("cq"))
        q4 = dot_nt(h_buf[0, b], cq4[...]).astype(BF16)
        for r in (3, 2, 1):
            q_snd[b, r - 1] = q4[:, r * 64:r * 64 + 64]
            start(q_snd.at[b, r - 1], q_rcv.at[b, c, span(y * 64, 64)], q_ssem.at[b, r - 1], q_rsem.at[b, r - 1], quad[r])
        q_rcv[b, c, span(y * 64, 64)] = q4[:, 0:64]
        if b == 0:
            send_weight("co", 3)
        else:
            for name in Y_SECOND:
                send_weight(name, 2)
        yield
        if b == 0:
            once(local[5].wait, local[6].wait)
        for half_id, pieces in ((c, (2,)), (1 - c, (1, 3))):
            for r in pieces:
                remote(q_snd.at[b, r - 1], q_rcv.at[b, quad_c[r], span(quad_y[r] * 64, 64)], q_ssem.at[b, r - 1], q_rsem.at[b, r - 1], quad[r]).wait_recv()
            o_buf[b, half_id] = cross(half_id, b)
            for r in reversed(pieces):
                start(o_buf.at[b, half_id, span(quad_y[r] * 64, 64)], o_rcv.at[b, r - 1], o_ssem.at[b, r - 1], o_rsem.at[b, r - 1], quad[r])
        if b == 1:
            for name in Y_THIRD:
                send_weight(name, 2)
            send_weight("wg", 3)
        yield
        for r in (1, 2, 3):
            remote(o_buf.at[b, quad_c[r], span(quad_y[r] * 64, 64)], o_rcv.at[b, r - 1], o_ssem.at[b, r - 1], o_rsem.at[b, r - 1], quad[r]).wait_recv()
        heads[b] = jnp.concatenate([o_buf[b, c, span(y * 64, 64), :]] + [o_rcv[b, r] for r in range(3)], axis=1)
        if b == 0:
            once(local[7].wait, *weight_waits("co"))
        partial = dot_nn(heads[b], co4[...])
        total = yield from reduce_scatter(1, b, partial, (lambda: send_weight("wu", 3)) if b == 1 else None)
        resid = resid + total
        h_buf[1, b, chunk(0, z)] = rms_norm(resid, nm_ref[...])
        yield from gather(1, b, (lambda: send_weight("wv", 3)) if b == 1 else None)
        if b == 0:
            send_weight("wd", 3)
            once(*[copy.wait for copy in local[8:]], *weight_waits("wg", "wu", "wv"))
        h = h_buf[1, b]
        act[b] = (gelu_tanh(dot_nt(h, wg4[...])) * dot_nt(h, wu4[...])).astype(BF16)
        if b == 0:
            once(*weight_waits("wd"))
        total = yield from reduce_scatter(2, b, dot_nn(act[b], wd4[...]))
        resid = resid + total
        out_ref[chunk(c * 256 + b * 128 + y * 64, z)] = resid.astype(BF16)
        yield from gather_out(b)

    flows = [flow(0), flow(1)]
    while flows:
        for item in list(flows):
            try:
                next(item)
            except StopIteration:
                flows.remove(item)
    for b in range(2):
        for s in range(8):
            yy = y if s < 4 else 1 - y
            part = out_ref.at[chunk((1 - c) * 256 + b * 128 + yy * 64, lax.rem(z + 4 - s % 4, 4))]
            remote(part, part, cs_sem.at[b, s], cr_sem.at[b, s], quad[1]).wait_recv()
    for copy in sends:
        copy.wait_send()


def tail(x_in, attn, mask_t, ck_t, cv_t, wo, cq_t, co, wg_t, wu_t, wd, woy, nc, nm):
    hbm = pl.BlockSpec(memory_space=pltpu.HBM)
    vmem = pl.BlockSpec(memory_space=pltpu.VMEM)
    units, wide = wd.shape
    deep = wo.shape[0]
    dma = pltpu.SemaphoreType.DMA
    bf16_shapes = [(2, 16, wide), ck_t.shape, cv_t.shape] + [(4 * deep, wide)] * 3 + [(4 * units, wide)] * 3
    bf16_shapes += [(2, 3, 64, deep), (2, 64, 4 * deep), (2, 3, 64, deep), (2, 2, 128, deep), (2, 2, 128, deep), (2, 3, 64, deep)]
    z_shapes = [(3, 2, 64, wide), (3, 2, 3, 16, wide), (2, 2, 64, wide), (2, 64, 4 * units)]
    sems = [(11,), (2,), (2,), (6, 3), (6, 3)] + [(2, 3)] * 6 + [(3, 2, 3)] * 4 + [(2, 4)] * 2 + [(2, 8)] * 2
    scratch = [pltpu.VMEM(shape, BF16) for shape in bf16_shapes]
    scratch += [pltpu.VMEM((deep, 128), F32), pltpu.VMEM((2, 64, wide), F32)]
    scratch += [pltpu.VMEM(shape, BF16) for shape in z_shapes] + [dma(shape) for shape in sems]
    return pl.pallas_call(
        tail_kernel,
        out_shape=jax.ShapeDtypeStruct(x_in.shape, BF16),
        in_specs=[hbm, vmem, vmem, hbm, hbm, vmem] + [hbm] * 6 + [vmem, vmem],
        out_specs=vmem,
        scratch_shapes=scratch,
        compiler_params=pltpu.CompilerParams(collective_id=0, has_side_effects=True, vmem_limit_bytes=50 * 2**20),
        name="tail",
    )(x_in, attn, mask_t, ck_t, cv_t, wo, cq_t, co, wg_t, wu_t, wd, woy, nc, nm)


def head_kernel(tok_ref, rb_ref, x_ref, wq_ref, wk_ref, wv_ref, ns_ref, k_hbm, v_hbm,
                attn_ref, nk_hbm, nv_hbm,
                kbuf, vbuf, h_buf, qq, k_new, v_new, table, in_sem, out_sem):
    rows, depth, t_len = kbuf.shape
    n_chunks = in_sem.shape[1]
    size = rows // n_chunks

    def chunk_copy(i, which):
        hbm, buf = ((k_hbm, kbuf), (v_hbm, vbuf))[which]
        part = pl.ds(i * size, size)
        return pltpu.make_async_copy(hbm.at[part], buf.at[part], in_sem.at[which, i])

    def chunk_out(i, which):
        hbm, buf = ((nk_hbm, kbuf), (nv_hbm, vbuf))[which]
        part = pl.ds(i * size, size)
        return pltpu.make_async_copy(buf.at[part], hbm.at[part], out_sem.at[which, i])

    for i in range(n_chunks):
        chunk_copy(i, 0).start()
        chunk_copy(i, 1).start()

    distance = lax.broadcasted_iota(jnp.int32, (t_len, t_len), 0) - lax.broadcasted_iota(jnp.int32, (t_len, t_len), 1)
    bias = jnp.full((t_len, t_len), rb_ref[0], F32)
    for bucket, edge in enumerate(BUCKET_EDGES):
        bias = jnp.where(distance >= edge, rb_ref[bucket + 1], bias)
    table[...] = jnp.where(distance >= 0, bias, NEG_FILL)

    wqq = jnp.concatenate([wq_ref[...], wq_ref[...]], axis=0)
    for i in range(rows // 128):
        part = slice(i * 128, i * 128 + 128)
        h = rms_norm(x_ref[part, :].astype(F32), ns_ref[...])
        qq[part, :] = dot_nt(h, wqq).astype(BF16).astype(F32)
        k_new[i] = dot_nt(wk_ref[...], h).astype(BF16).astype(F32)
        v_new[i] = dot_nt(wv_ref[...], h).astype(BF16).astype(F32)

    lane = lax.broadcasted_iota(jnp.int32, (depth, t_len), 1)
    row8 = lax.broadcasted_iota(jnp.int32, (8, 128), 0)
    half8 = lax.broadcasted_iota(jnp.int32, (8, 128), 1) // depth

    def step(i, carry):
        chunk_copy(i, 0).wait()
        chunk_copy(i, 1).wait()
        k_cols, v_cols = k_new[i], v_new[i]
        scores = []
        for g in range(size // 8):
            k8, bias8 = [], []
            for j in range(8):
                b = i * size + g * 8 + j
                pos = tok_ref[b]
                at_pos = lane == pos
                col = g * 8 + j
                k_b = jnp.where(at_pos, pltpu.roll(k_cols, pos + (t_len - col), 1), kbuf[b].astype(F32)).astype(BF16)
                v_b = jnp.where(at_pos, pltpu.roll(v_cols, pos + (t_len - col), 1), vbuf[b].astype(F32)).astype(BF16)
                kbuf[b] = k_b
                vbuf[b] = v_b
                k8.append(k_b)
                bias8.append(table[pl.ds(pos, 1), :])
            q8 = qq[pl.ds(pl.multiple_of(i * size + g * 8, 8), 8), :]
            q_diag = jnp.concatenate([jnp.where(row8 == 2 * m + half8, q8, 0.0) for m in range(4)], axis=1).astype(BF16)
            scores.append(dot_nn(q_diag, jnp.concatenate(k8, axis=0)) + jnp.concatenate(bias8, axis=0))
        chunk_out(i, 0).start()
        chunk_out(i, 1).start()
        s = jnp.concatenate(scores, axis=0)
        e = jnp.exp(s - jnp.max(s, axis=1, keepdims=True))
        p = (e / jnp.sum(e, axis=1, keepdims=True)).astype(BF16).astype(F32)
        outs = []
        for g in range(size // 8):
            p8 = p[g * 8:g * 8 + 8, :]
            p_diag = jnp.concatenate([jnp.where(row8 == j, p8, 0.0) for j in range(8)], axis=1).astype(BF16)
            v8 = jnp.concatenate([vbuf[i * size + g * 8 + j] for j in range(8)], axis=1)
            outs.append(dot_nt(p_diag, v8))
        attn_ref[pl.ds(pl.multiple_of(i * size, size), size), :] = jnp.concatenate(outs, axis=0).astype(BF16)
        return carry

    lax.fori_loop(0, n_chunks, step, 0)
    for i in range(n_chunks):
        chunk_out(i, 0).wait()
        chunk_out(i, 1).wait()


def head(tok_pos, rel_bias, x_in, wq_t, wk_t, wv_t, ns, k_t, v_t):
    hbm = pl.BlockSpec(memory_space=pltpu.HBM)
    vmem = pl.BlockSpec(memory_space=pltpu.VMEM)
    smem = pl.BlockSpec(memory_space=pltpu.SMEM)
    rows, depth, t_len = k_t.shape
    dma = pltpu.SemaphoreType.DMA
    n_chunks = 4
    return pl.pallas_call(
        head_kernel,
        out_shape=(jax.ShapeDtypeStruct((rows, depth), BF16), jax.ShapeDtypeStruct(k_t.shape, BF16), jax.ShapeDtypeStruct(v_t.shape, BF16)),
        in_specs=[smem, smem] + [vmem] * 5 + [hbm] * 2,
        out_specs=(vmem, hbm, hbm),
        scratch_shapes=[
            pltpu.VMEM(k_t.shape, BF16), pltpu.VMEM(v_t.shape, BF16), pltpu.VMEM((8, 128), BF16),
            pltpu.VMEM((rows, 2 * depth), F32), pltpu.VMEM((rows // 128, depth, 128), F32), pltpu.VMEM((rows // 128, depth, 128), F32),
            pltpu.VMEM((t_len, t_len), F32), dma((2, n_chunks)), dma((2, n_chunks)),
        ],
        compiler_params=pltpu.CompilerParams(vmem_limit_bytes=VMEM_BYTES),
        cost_estimate=pl.CostEstimate(flops=4 * 10**9, bytes_accessed=34 * 2**20, transcendentals=2**16),
        name="head",
    )(tok_pos, rel_bias, x_in, wq_t, wk_t, wv_t, ns, k_t, v_t)


def solution(mesh):
    def local_layer(x_in, tok_pos, self_k, self_v, cross_k, cross_v, enc_mask, rel_bias, w_q, w_k, w_v, w_o, cross_q, cross_o, w_gate, w_up, w_down, norm_self, norm_cross, norm_mlp):
        k_t = jnp.transpose(self_k[:, :, 0, :], (0, 2, 1))
        v_t = jnp.transpose(self_v[:, :, 0, :], (0, 2, 1))
        attn, new_k, new_v = head(tok_pos, rel_bias[:, 0], x_in, w_q.T, w_k.T, w_v.T, norm_self, k_t, v_t)
        new_self_k = jnp.transpose(new_k, (0, 2, 1))[:, :, None, :]
        new_self_v = jnp.transpose(new_v, (0, 2, 1))[:, :, None, :]
        ck_t = jnp.transpose(cross_k[:, :, 0, :], (1, 2, 0))
        cv_t = jnp.transpose(cross_v[:, :, 0, :], (1, 2, 0))
        wo_y = lax.ppermute(w_o, "tp", [(i, i ^ 2) for i in range(mesh.shape["tp"])])
        out = tail(x_in, attn, enc_mask.T, ck_t, cv_t, w_o, cross_q.T, cross_o, w_gate.T, w_up.T, w_down, wo_y, norm_cross, norm_mlp)
        return out, new_self_k, new_self_v

    cache_spec = P('dp', None, 'tp', None)
    split_cols = P(None, 'tp')
    split_rows = P('tp', None)
    in_specs = (P('dp', None), P('dp'), cache_spec, cache_spec, cache_spec, cache_spec, P('dp', None), split_cols, split_cols, split_cols, split_cols, split_rows, split_cols, split_rows, split_cols, split_cols, split_rows, P(None), P(None), P(None))
    out_specs = (P('dp', None), cache_spec, cache_spec)
    return jax.shard_map(local_layer, mesh=mesh, in_specs=in_specs, out_specs=out_specs, check_vma=False)
```
